32 devices in a mesh: dp: 8 (over z, core), mp: 4 (over y, x).
Axes of the slice: x: 2, y: 2, z: 4, core: 2. Of those that a mesh axis runs over, the one named last changes fastest.
Arguments:
- patches: bfloat16 [256, 256, 1280], P(('dp', 'mp')), may hold values from -6 to 6
- position: bfloat16 [256, 1280], replicated, may hold values from -3 to 3
- keep: int32 [256, 64], P(('dp', 'mp')), may hold values from 0 to 255, as said below
- counts: int32 [256], replicated, may hold values from 1 to 64, as said below
- offsets: int32 [256], replicated, may hold values from 0 to 10239, as said below
- ln_gain: float32 [1, 2, 1280], replicated, may hold values from 0.25 to 1.75
- ln_bias: float32 [1, 2, 1280], replicated, may hold values from -2 to 2
- w_qkv: bfloat16 [1, 3, 1280, 1280], P(None, None, 'dp', 'mp')
- b_qkv: float32 [1, 3, 1280], P(None, None, 'mp'), may hold values from -3 to 3
- w_o: bfloat16 [1, 1280, 1280], P(None, 'mp', 'dp'), may hold values from -0.15625 to 0.15625
- b_o: float32 [1, 1280], replicated, may hold values from -1.5 to 1.5
- w_up: bfloat16 [1, 1280, 5120], P(None, 'dp', 'mp'), may hold values from -0.15625 to 0.15625
- b_up: float32 [1, 5120], P(None, 'mp'), may hold values from -3 to 3
- w_down: bfloat16 [1, 5120, 1280], P(None, 'mp', 'dp'), may hold values from -0.078125 to 0.078125
- b_down: float32 [1, 1280], replicated, may hold values from -1.5 to 1.5
Outputs:
- encoded: bfloat16 [10240, 1280], P(('dp', 'mp'))
The draws below stay inside these ranges and needn't reach their ends.
Inputs may be any that keep to these rules, and one draw needn't show every extreme that they name: `keep`: the first counts[i] entries of row i are distinct and name image i's visible patches; later entries are unused. `counts`: some image has exactly 64 visible patches. Image i, held by dp index s = i // 32, occupies packed rows offsets[i] to offsets[i] + counts[i] - 1, all inside the aligned block of 160 rows numbered d * 8 + s for some shard d; no two images share a row.
All inputs are finite; a program needn't handle non-finite values.
Results may differ from the reference program's by a relative error of at most 0.015.
Values may be sent and summed in bfloat16 or wider, within the bound.
No kernel may reach another device: no remote copies, remote signals or barrier semaphores. Data moves between devices by JAX's collectives and lax.ppermute only.
A program may use at most 64 MiB of HBM per device.

```python
import math
import jax
import jax.numpy as jnp
from jax import lax

D = 1280
HEADS = 16
HEAD = 80
FF = 5120
PATCHES = 256
KEEP_MAX = 64
LAYERS = 1
IMG_DEV = 32
IMAGES = 256
SLOT = 160
PACK_DEV = 1280
PACKED = 10240
N_MP = 4


def packing_plan(key):
    shard_total = IMAGES // IMG_DEV
    key_order, key_raw, key_cap, key_force = jax.random.split(jax.random.fold_in(key, 71), 4)
    order = jax.vmap(lambda subkey: jax.random.permutation(subkey, IMG_DEV))(jax.random.split(key_order, shard_total)).astype(jnp.int32)
    destination = order % shard_total
    rank_in = order // shard_total
    lowest = max(1, KEEP_MAX // 8)
    ceiling = jax.random.randint(key_cap, (shard_total, 1), lowest, KEEP_MAX + 1)
    raw_count = jnp.minimum(jax.random.randint(key_raw, (shard_total, IMG_DEV), lowest, KEEP_MAX + 1), ceiling)
    mates = destination[:, :, None] == destination[:, None, :]
    mate_total = jnp.sum(jnp.where(mates, raw_count[:, None, :], 0), axis=-1)
    mate_number = jnp.sum(mates.astype(jnp.int32), axis=-1)
    room = SLOT - mate_number
    scaled = 1 + (raw_count - 1) * room // jnp.maximum(mate_total - mate_number, room)
    forced_source = jax.random.randint(key_force, (), 0, shard_total)
    source_ids = jnp.arange(shard_total, dtype=jnp.int32)[:, None]
    in_source = source_ids == forced_source
    chosen = in_source & (order == 0)
    partner = in_source & (destination == 0)
    counts_grid = jnp.where(chosen, KEEP_MAX, jnp.where(partner, 1, scaled))
    earlier = mates & (rank_in[:, None, :] < rank_in[:, :, None])
    before = jnp.sum(jnp.where(earlier, counts_grid[:, None, :], 0), axis=-1)
    offsets_grid = destination * PACK_DEV + source_ids * SLOT + before
    return (counts_grid.reshape(IMAGES).astype(jnp.int32), offsets_grid.reshape(IMAGES).astype(jnp.int32))


def draw_counts(key, part):
    return packing_plan(key)[0]


def draw_offsets(key, part):
    return packing_plan(key)[1]


def draw_keep(key, part):
    subkeys = jax.random.split(jax.random.fold_in(key, 13), IMAGES)
    return jax.vmap(lambda subkey: jax.random.permutation(subkey, PATCHES)[:KEEP_MAX])(subkeys).astype(jnp.int32)


def draw_w_qkv(key, part):
    key_base = jax.random.fold_in(jax.random.fold_in(key, 29), 0)
    matrices = jax.random.normal(key_base, (LAYERS, 3, D, D), jnp.float32) / math.sqrt(D)
    return matrices.astype(jnp.bfloat16)


def levels(rng, extent, cuts, low, largest):
    level, own = 1.0, jax.random.fold_in(rng, 6)
    for dim, blocks in cuts:
        steps = jnp.exp(jax.random.uniform(jax.random.fold_in(own, dim), (blocks,), jnp.float32, low / len(cuts), largest / len(cuts)))
        level = level * jnp.repeat(steps, extent[dim] // blocks).reshape([-1 if axis == dim else 1 for axis in range(len(extent))])
    return level


def bell_draw(rng, extent, deviation, limit, cuts=(), kind=jnp.bfloat16):
    result = jax.random.normal(rng, extent, jnp.float32) * deviation
    if len(cuts) > 0:
        result = levels(rng, extent, cuts, -0.22, 0.18) * result
    return jnp.clip(result, min=-limit, max=limit).astype(kind)


def setup_inputs(seed: int = 0) -> dict:
    keys = jax.random.split(jax.random.key(seed), 16)
    return {
        "patches": bell_draw(keys[0], (IMAGES, PATCHES, D), 1.0, 6.0, ((0, 32),)),
        "position": bell_draw(keys[1], (PATCHES, D), 0.5, 3.0),
        "keep": draw_keep(jax.random.fold_in(keys[15], 71), 0),
        "counts": draw_counts(jax.random.fold_in(keys[15], 71), 0),
        "offsets": draw_offsets(jax.random.fold_in(keys[15], 71), 0),
        "ln_gain": jnp.clip(1.0 + 0.15 * jax.random.normal(keys[5], (LAYERS, 2, D), jnp.float32), 0.25, 1.75),
        "ln_bias": bell_draw(keys[6], (LAYERS, 2, D), 0.3, 2.0, (), jnp.float32),
        "w_qkv": draw_w_qkv(jax.random.fold_in(keys[15], 71), 0),
        "b_qkv": bell_draw(keys[8], (LAYERS, 3, D), 0.5, 3.0, ((2, 4),), jnp.float32),
        "w_o": bell_draw(keys[9], (LAYERS, D, D), D ** -0.5, 0.15625, ((1, 4), (2, 8))),
        "b_o": bell_draw(keys[10], (LAYERS, D), 0.2, 1.5, (), jnp.float32),
        "w_up": bell_draw(keys[11], (LAYERS, D, FF), D ** -0.5, 0.15625, ((1, 8), (2, 4))),
        "b_up": bell_draw(keys[12], (LAYERS, FF), 0.5, 3.0, ((1, 4),), jnp.float32),
        "w_down": bell_draw(keys[13], (LAYERS, FF, D), FF ** -0.5, 0.078125, ((1, 4), (2, 8))),
        "b_down": bell_draw(keys[14], (LAYERS, D), 0.2, 1.5, (), jnp.float32),
    }


def layer_norm(values, gain_row, shift_row):
    row_mean = lax.optimization_barrier(jnp.mean(values, axis=-1, keepdims=True))
    centred = values - row_mean
    spread = lax.optimization_barrier(jnp.mean(centred * centred, axis=-1, keepdims=True))
    return (centred * lax.rsqrt(spread + 1e-06) * gain_row + shift_row).astype(jnp.bfloat16)

def split_sum(left, weight, groups):
    group_width = left.shape[1] // groups
    running = jnp.zeros((left.shape[0], weight.shape[1]), jnp.float32)
    for group_index in range(groups):
        partial_value = jnp.dot(left[:, group_index * group_width:(group_index + 1) * group_width], weight[group_index * group_width:(group_index + 1) * group_width], preferred_element_type=jnp.float32)
        rounded = lax.optimization_barrier(partial_value.astype(jnp.bfloat16))
        running = running + rounded.astype(jnp.float32)
    return running

def shard_attention(pieces):
    queries, key_rows, value_rows, labels_shard = pieces
    scores = jnp.einsum('qhe,khe->hqk', queries.astype(jnp.float32), key_rows.astype(jnp.float32)) * (1.0 / math.sqrt(HEAD))
    matches = labels_shard[:, None] == labels_shard[None, :]
    scores = jnp.where(matches[None], scores, -jnp.inf)
    row_max = lax.optimization_barrier(jnp.max(scores, axis=-1, keepdims=True))
    weights = jnp.exp(scores - row_max)
    probabilities = (weights / lax.optimization_barrier(jnp.sum(weights, axis=-1, keepdims=True))).astype(jnp.bfloat16)
    attended = jnp.einsum('hqk,khe->qhe', probabilities.astype(jnp.float32), value_rows.astype(jnp.float32))
    return attended.astype(jnp.bfloat16)

def reference(patches, position, keep, counts, offsets, ln_gain, ln_bias, w_qkv, b_qkv, w_o, b_o, w_up, b_up, w_down, b_down):
    picked = jnp.take_along_axis(patches, keep[:, :, None], axis=1)
    placed = jnp.take(position, keep, axis=0)
    tokens = (picked.astype(jnp.float32) + placed.astype(jnp.float32)).astype(jnp.bfloat16)
    positions_in = jnp.arange(KEEP_MAX, dtype=jnp.int32)
    is_live = positions_in[None, :] < counts[:, None]
    target = jnp.where(is_live, offsets[:, None] + positions_in[None, :], PACKED).reshape(-1)
    stream = jnp.zeros((PACKED, D), jnp.bfloat16).at[target].set(tokens.reshape(-1, D), mode='drop')
    packed_rows = jnp.arange(PACKED, dtype=jnp.int32)
    image_ids = jnp.arange(counts.shape[0], dtype=jnp.int32)
    inside = (packed_rows[:, None] >= offsets[None, :]) & (packed_rows[:, None] < (offsets + counts)[None, :])
    labels = lax.optimization_barrier(jnp.max(jnp.where(inside, image_ids[None, :] + 1, 0), axis=1)) - 1
    shard_total = PACKED // PACK_DEV
    for layer_index in range(LAYERS):
        normed = layer_norm(stream.astype(jnp.float32), ln_gain[layer_index, 0], ln_bias[layer_index, 0])
        projected = (jnp.einsum('rd,tdc->trc', normed.astype(jnp.float32), w_qkv[layer_index].astype(jnp.float32)) + b_qkv[layer_index][:, None, :]).astype(jnp.bfloat16)
        shaped = projected.reshape(3, shard_total, PACK_DEV, HEADS, HEAD)
        attended = lax.map(shard_attention, (shaped[0], shaped[1], shaped[2], labels.reshape(shard_total, PACK_DEV)))
        attended = attended.reshape(PACKED, D)
        residual = stream.astype(jnp.float32) + split_sum(attended, w_o[layer_index], N_MP) + b_o[layer_index]
        normed_mlp = layer_norm(residual, ln_gain[layer_index, 1], ln_bias[layer_index, 1])
        up_proj = jnp.dot(normed_mlp, w_up[layer_index], preferred_element_type=jnp.float32) + b_up[layer_index]
        hidden = jax.nn.gelu(up_proj, approximate=False).astype(jnp.bfloat16)
        stream = (residual + split_sum(hidden, w_down[layer_index], N_MP) + b_down[layer_index]).astype(jnp.bfloat16)
    return jnp.where(labels[:, None] >= 0, stream, jnp.zeros_like(stream))
```

```python
import functools
import math

import jax
import jax.numpy as jnp
from jax import lax
from jax.experimental import pallas as pl
from jax.experimental.pallas import tpu as pltpu
from jax.sharding import PartitionSpec as P

HEAD = 80
LANES = 128
BF = jnp.bfloat16
F32 = jnp.float32
NT = (((1,), (1,)), ((), ()))


def cost(flops, moved):
    return pl.CostEstimate(flops=int(flops), bytes_accessed=int(moved), transcendentals=0)


def params(mib=48):
    return pltpu.CompilerParams(vmem_limit_bytes=mib * 1024 * 1024)


def embed_kernel(keep_ref, patches_ref, position_ref, out_ref):
    per, patch_count, width = patches_ref.shape
    row = keep_ref[0].astype(F32)
    tokens = row.shape[1]
    kept = jnp.broadcast_to(row, (tokens, tokens)).T
    reps = (patch_count + tokens - 1) // tokens
    wide = jnp.concatenate([kept] * reps, axis=1)[:, :patch_count]
    lane = lax.broadcasted_iota(jnp.int32, (tokens, patch_count), 1).astype(F32)
    onehot = jnp.where(wide == lane, 1.0, 0.0).astype(BF)
    each = tokens // per
    placed = jnp.dot(onehot, position_ref[...], preferred_element_type=F32)
    picked = jnp.concatenate(
        [
            jnp.dot(onehot[i * each : (i + 1) * each], patches_ref[i], preferred_element_type=F32)
            for i in range(per)
        ],
        axis=0,
    )
    out_ref[...] = (picked + placed).T.astype(BF).reshape(out_ref.shape)


def embed(patches, position, keep, n_mp):
    images, patch_count, width = patches.shape
    keep_most = keep.shape[1]
    per = max(1, min(images, LANES // keep_most))
    steps = images // per
    tokens = per * keep_most
    return pl.pallas_call(
        embed_kernel,
        grid=(steps,),
        in_specs=[
            pl.BlockSpec((1, 1, tokens), lambda i: (i, 0, 0)),
            pl.BlockSpec((per, patch_count, width), lambda i: (i, 0, 0)),
            pl.BlockSpec((patch_count, width), lambda i: (0, 0)),
        ],
        out_specs=pl.BlockSpec((n_mp, width // n_mp, tokens), lambda i: (0, 0, i)),
        out_shape=jax.ShapeDtypeStruct((n_mp, width // n_mp, images * keep_most), BF),
        compiler_params=params(),
        cost_estimate=cost(4e9, patches.size * 2),
        name="embed",
    )(keep.reshape(steps, 1, tokens), patches, position)


def pack_kernel(parts, fold, slot_rows, target_ref, feat_ref, *out_refs):
    n_src, width, tokens = feat_ref.shape
    here = out_refs[0].shape[0]
    rows = here * slot_rows
    first = pl.program_id(0) * rows
    row = lax.broadcasted_iota(jnp.int32, (rows, tokens), 0) + first
    total = jnp.zeros((rows, width), F32)
    for j in range(n_src):
        onehot = jnp.where(row == target_ref[j], 1.0, 0.0).astype(BF)
        total = total + lax.dot_general(onehot, feat_ref[j], NT, preferred_element_type=F32)
    piece = slot_rows // (parts * fold)
    for s in range(here):
        for p in range(parts):
            start = s * slot_rows + p * fold * piece
            chunks = [total[start + f * piece : start + (f + 1) * piece] for f in range(fold)]
            out_refs[p][s] = jnp.concatenate(chunks, axis=1).astype(BF)


def pack(featured, target, slots, slot_rows, parts, fold):
    n_src, width, tokens = featured.shape
    steps = 2
    piece = slot_rows // (parts * fold)
    return pl.pallas_call(
        functools.partial(pack_kernel, parts, fold, slot_rows),
        grid=(steps,),
        in_specs=[
            pl.BlockSpec((n_src, 1, tokens), lambda i: (0, 0, 0)),
            pl.BlockSpec((n_src, width, tokens), lambda i: (0, 0, 0)),
        ],
        out_specs=[pl.BlockSpec((slots // steps, piece, fold * width), lambda i: (i, 0, 0))] * parts,
        out_shape=[jax.ShapeDtypeStruct((slots, piece, fold * width), BF)] * parts,
        compiler_params=params(),
        cost_estimate=cost(4e9, featured.size * 2),
        name="pack",
    )(target, featured)


def unfold(refs, fold):
    slots = refs[0].shape[0]
    width = refs[0].shape[2] // fold
    pieces = []
    for s in range(slots):
        for ref in refs:
            values = ref[s].astype(F32)
            for f in range(fold):
                pieces.append(values[:, f * width : (f + 1) * width])
    return jnp.concatenate(pieces, axis=0)


def attend_kernel(n_mp, parts, fold, hc, m_ref, *refs):
    gathered = [refs[k * parts : (k + 1) * parts] for k in range(n_mp)]
    weight_ref, bias_ref, gain_ref, shift_ref, labrow_ref, labcol_ref = refs[
        n_mp * parts : n_mp * parts + 6
    ]
    out_refs = refs[n_mp * parts + 6 :]
    me = m_ref[0]
    blocks = [unfold(g, fold) for g in gathered]
    rows, width = blocks[0].shape
    full = width * n_mp
    mean = sum(jnp.sum(b, axis=1, keepdims=True) for b in blocks) * (1.0 / full)
    blocks = [b - mean for b in blocks]
    spread = sum(jnp.sum(b * b, axis=1, keepdims=True) for b in blocks) * (1.0 / full)
    scale = lax.rsqrt(spread + 1e-06)
    qkv = jnp.zeros((rows, 3 * hc), F32)
    for k in range(n_mp):
        which = jnp.bitwise_xor(me, k)
        normed = (blocks[k] * scale * gain_ref[which] + shift_ref[which]).astype(BF)
        rows_w = pl.ds(pl.multiple_of(which * width, 32), width)
        qkv = qkv + jnp.dot(normed, weight_ref[rows_w, : 3 * hc], preferred_element_type=F32)
    qkv = (qkv + bias_ref[...]).astype(BF)
    query, key, value = (qkv[:, t * hc : (t + 1) * hc] for t in range(3))
    slots = len(out_refs)
    slot_rows = rows // slots
    heads = hc // HEAD
    lane_head = lax.broadcasted_iota(jnp.int32, (slot_rows, hc), 1) // HEAD
    start = (3 * hc) // LANES * LANES
    lead = 3 * hc - start
    for s in range(slots):
        at = slice(s * slot_rows, (s + 1) * slot_rows)
        q, kk, v = query[at], key[at], value[at]
        zero = jnp.zeros_like(q)
        stacked = jnp.concatenate([jnp.where(lane_head == h, q, zero) for h in range(heads)], axis=0)
        scores = lax.dot_general(stacked, kk, NT, preferred_element_type=F32)
        scores = scores * (1.0 / math.sqrt(HEAD))
        same = labcol_ref[s] == labrow_ref[s]
        outs = jnp.zeros((slot_rows, hc), F32)
        for h in range(heads):
            sh = jnp.where(same, scores[h * slot_rows : (h + 1) * slot_rows], -jnp.inf)
            e = jnp.exp(sh - jnp.max(sh, axis=1, keepdims=True))
            prob = (e / jnp.sum(e, axis=1, keepdims=True)).astype(BF)
            outs = jnp.where(
                lane_head == h, jnp.dot(prob, v, preferred_element_type=F32), outs
            )
        if lead:
            outs = jnp.concatenate([jnp.zeros((slot_rows, lead), F32), outs], axis=1)
        out_refs[s][...] = lax.dot_general(
            outs.astype(BF), weight_ref[:, start:], NT, preferred_element_type=F32
        ).astype(BF)


def attend(dest, me, gathered, parts, fold, hc, weight, bias, gain, shift, labrow, labcol, spm):
    n_mp = len(gathered) // parts
    slots, piece, lanes = gathered[0].shape
    slot_rows = labrow.shape[2]
    width = weight.shape[0]

    def block(i, m):
        return (jnp.bitwise_xor(m[0], dest), 0, 0)

    def whole(rank):
        return lambda i, m: (0,) * rank

    feat = lanes // fold
    return pl.pallas_call(
        functools.partial(attend_kernel, n_mp, parts, fold, hc),
        grid_spec=pltpu.PrefetchScalarGridSpec(
            num_scalar_prefetch=1,
            grid=(1,),
            in_specs=[pl.BlockSpec((spm, piece, lanes), block)] * len(gathered)
            + [
                pl.BlockSpec(weight.shape, whole(2)),
                pl.BlockSpec(bias.shape, whole(2)),
                pl.BlockSpec((n_mp, 1, feat), whole(3)),
                pl.BlockSpec((n_mp, 1, feat), whole(3)),
                pl.BlockSpec((spm, 1, slot_rows), block),
                pl.BlockSpec((spm, slot_rows, 1), block),
            ],
            out_specs=[pl.BlockSpec((slot_rows, width), whole(2))] * spm,
        ),
        out_shape=[jax.ShapeDtypeStruct((slot_rows, width), BF)] * spm,
        compiler_params=params(),
        cost_estimate=cost(4e9, weight.size * 2),
        name=f"attend_{dest}",
    )(me, *gathered, weight, bias, gain, shift, labrow, labcol)


def residual_kernel(n_mp, parts, fold, adds, m_ref, *refs):
    gathered = [refs[k * parts : (k + 1) * parts] for k in range(n_mp)]
    rest = refs[n_mp * parts :]
    add_refs, (bias_ref, gain_ref, shift_ref) = rest[:adds], rest[adds : adds + 3]
    res_ref, out_refs = rest[adds + 3], rest[adds + 4 :]
    me = m_ref[0]
    blocks = [unfold(g, fold) for g in gathered]
    ordered = []
    for j in range(n_mp):
        value = blocks[0]
        for k in range(1, n_mp):
            value = jnp.where(jnp.bitwise_xor(me, k) == j, blocks[k], value)
        ordered.append(value)
    rows = jnp.concatenate(ordered, axis=1)
    slots = len(out_refs)
    slot_rows = rows.shape[0] // slots
    for s in range(slots):
        value = rows[s * slot_rows : (s + 1) * slot_rows] + bias_ref[...]
        for i in range(s, adds, slots):
            value = value + add_refs[i][...].astype(F32)
        res_ref[s] = value
        mean = jnp.mean(value, axis=1, keepdims=True)
        value = value - mean
        spread = jnp.mean(value * value, axis=1, keepdims=True)
        out_refs[s][...] = (
            value * lax.rsqrt(spread + 1e-06) * gain_ref[...] + shift_ref[...]
        ).astype(BF)


def residual_norm(me, gathered, parts, fold, added, bias, gain, shift, spm):
    n_mp = len(gathered) // parts
    slots, piece, lanes = gathered[0].shape
    slot_rows, width = added[0].shape

    def block(i, m):
        return (m[0], 0, 0)

    def whole(rank):
        return lambda i, m: (0,) * rank

    row = pl.BlockSpec((1, width), whole(2))
    return pl.pallas_call(
        functools.partial(residual_kernel, n_mp, parts, fold, len(added)),
        grid_spec=pltpu.PrefetchScalarGridSpec(
            num_scalar_prefetch=1,
            grid=(1,),
            in_specs=[pl.BlockSpec((spm, piece, lanes), block)] * len(gathered)
            + [pl.BlockSpec((slot_rows, width), whole(2))] * len(added)
            + [row] * 3,
            out_specs=[pl.BlockSpec((spm, slot_rows, width), whole(3))]
            + [pl.BlockSpec((slot_rows, width), whole(2))] * spm,
        ),
        out_shape=[jax.ShapeDtypeStruct((spm, slot_rows, width), F32)]
        + [jax.ShapeDtypeStruct((slot_rows, width), BF)] * spm,
        compiler_params=params(),
        cost_estimate=cost(1e9, 4 * spm * slot_rows * width * 4),
        name="residual_norm",
    )(me, *gathered, *added, bias, gain, shift)


def mlp_kernel(spm, *refs):
    in_refs, (up_ref, bias_ref, down_ref), out_refs = refs[:spm], refs[spm : spm + 3], refs[spm + 3 :]
    rows = jnp.concatenate([r[...] for r in in_refs], axis=0)
    slot_rows = in_refs[0].shape[0]
    hidden_width = up_ref.shape[1]
    step = min(256, hidden_width)
    total = jnp.zeros((rows.shape[0], down_ref.shape[0]), F32)
    for c in range(0, hidden_width, step):
        at = slice(c, c + step)
        up = jnp.dot(rows, up_ref[:, at], preferred_element_type=F32) + bias_ref[:, at]
        hidden = (0.5 * up * (1.0 + lax.erf(up * math.sqrt(0.5)))).astype(BF)
        total = total + lax.dot_general(
            hidden, down_ref[:, at], NT, preferred_element_type=F32
        )
    total = total.astype(BF)
    for s in range(spm):
        out_refs[s][...] = total[s * slot_rows : (s + 1) * slot_rows]


def mlp(rows, up, bias, down, dest):
    spm = len(rows)
    slot_rows, width = rows[0].shape
    return pl.pallas_call(
        functools.partial(mlp_kernel, spm),
        out_shape=[jax.ShapeDtypeStruct((slot_rows, down.shape[0]), BF)] * spm,
        compiler_params=params(),
        cost_estimate=cost(5e9, up.size * 4),
        name=f"mlp_{dest}",
    )(*rows, up, bias, down)


def finish_kernel(adds, *refs):
    add_refs, (res_ref, bias_ref, lab_ref, out_ref) = refs[:adds], refs[adds:]
    slots, slot_rows, width = res_ref.shape
    for s in range(slots):
        value = res_ref[s] + bias_ref[...]
        for i in range(s, adds, slots):
            value = value + add_refs[i][...].astype(F32)
        value = jnp.where(lab_ref[s] >= 0, value, 0.0)
        out_ref[s * slot_rows : (s + 1) * slot_rows] = value.astype(BF)


def finish(added, residual, bias, labels):
    slots, slot_rows, width = residual.shape
    return pl.pallas_call(
        functools.partial(finish_kernel, len(added)),
        out_shape=jax.ShapeDtypeStruct((slots * slot_rows, width), BF),
        compiler_params=params(),
        cost_estimate=cost(1e9, residual.size * 8),
        name="finish",
    )(*added, residual, bias, labels)


def hop(value, k, n):
    return lax.ppermute(value, "mp", [(i, i ^ k) for i in range(n)])


def gather_blocks(pieces, n):
    out = [list(pieces)] + [None] * (n - 1)
    if n != 4 or len(pieces) != 2:
        for k in range(1, n):
            out[k] = [hop(p, k, n) for p in pieces]
        return out
    x = [hop(pieces[0], 1, n), hop(pieces[1], 1, n)]
    y = [hop(pieces[0], 2, n), hop(pieces[1], 2, n)]
    out[1], out[2] = x, y
    out[3] = [hop(x[0], 2, n), hop(y[1], 1, n)]
    return out


def plus(a, b):
    return (a.astype(F32) + b.astype(F32)).astype(BF)


def scatter_blocks(partials, n):
    own = list(partials[0])
    if n != 4 or len(own) != 2:
        for k in range(1, n):
            own += [hop(p, k, n) for p in partials[k]]
        return own
    far, x, y = partials[3], partials[1], partials[2]
    first, second = hop(far[0], 1, n), hop(far[1], 2, n)
    x0, y1 = hop(x[0], 1, n), hop(y[1], 2, n)
    y0, x1 = hop(plus(y[0], first), 2, n), hop(plus(x[1], second), 1, n)
    return own + [x0, x1, y0, y1]


def per_device(
    patches,
    position,
    keep,
    counts,
    offsets,
    ln_gain,
    ln_bias,
    w_qkv,
    b_qkv,
    w_o,
    b_o,
    w_up,
    b_up,
    w_down,
    b_down,
):
    local_images, _, width = patches.shape
    keep_most = keep.shape[1]
    n_dp, n_mp = lax.axis_size("dp"), lax.axis_size("mp")
    d, m = lax.axis_index("dp"), lax.axis_index("mp")
    images_here = local_images * n_mp
    per_slot = (images_here + n_dp - 1) // n_dp
    slot_rows = max(keep_most + 16, per_slot * keep_most * 5 // 8)
    pack_rows = slot_rows * n_dp
    spm = n_dp // n_mp
    feat = width // n_mp
    hc = w_qkv.shape[3]
    me = m.astype(jnp.int32).reshape(1)

    mixed = jnp.concatenate([w_qkv[0, 0], w_qkv[0, 1], w_qkv[0, 2], w_o[0].T], axis=1)
    mixed = lax.all_gather(mixed, "dp", axis=0, tiled=True)
    up = lax.all_gather(w_up[0], "dp", axis=0, tiled=True)
    down = lax.all_gather(w_down[0].T, "dp", axis=0, tiled=True)

    tokens = embed(patches, position, keep, n_mp)
    featured = lax.all_to_all(tokens, "mp", split_axis=0, concat_axis=0, tiled=True)
    first_image = d * images_here
    group_counts = lax.dynamic_slice_in_dim(counts, first_image, images_here)
    group_offsets = lax.dynamic_slice_in_dim(offsets, first_image, images_here)
    shard_index = group_offsets // pack_rows
    base_row = shard_index * slot_rows + group_offsets - shard_index * pack_rows - d * slot_rows
    spot = jnp.arange(keep_most, dtype=jnp.int32)
    target = jnp.where(
        spot[None, :] < group_counts[:, None], base_row[:, None] + spot[None, :], pack_rows
    ).reshape(n_mp, 1, local_images * keep_most)
    parts = 2 if slot_rows % 32 == 0 else 1
    fold = 2
    packed = pack(featured, target, n_dp, slot_rows, parts, fold)
    packed = [
        lax.all_to_all(p, "dp", split_axis=0, concat_axis=0, tiled=True) for p in packed
    ]

    image_ids = jnp.arange(counts.shape[0], dtype=jnp.int32)
    packed_rows = d * pack_rows + jnp.arange(pack_rows, dtype=jnp.int32)
    inside = (packed_rows[:, None] >= offsets[None, :]) & (
        packed_rows[:, None] < (offsets + counts)[None, :]
    )
    labels = jnp.max(jnp.where(inside, image_ids[None, :] + 1, 0), axis=1) - 1
    labrow = labels.reshape(n_dp, 1, slot_rows)
    labcol = labels.reshape(n_dp, slot_rows, 1)

    gathered = sum(gather_blocks(packed, n_mp), [])
    gain = ln_gain[0, 0].reshape(n_mp, 1, feat)
    shift = ln_bias[0, 0].reshape(n_mp, 1, feat)
    bias = b_qkv[0].reshape(1, 3 * hc)
    order = [3, 1, 2, 0] if n_mp == 4 else list(range(n_mp))
    partials = [None] * n_mp
    for k in order:
        partials[k] = attend(
            k, me, gathered, parts, fold, hc, mixed, bias, gain, shift, labrow, labcol, spm
        )
    added = scatter_blocks(partials, n_mp)
    residual, *normed = residual_norm(
        me, gathered, parts, fold, added, b_o, ln_gain[0, 1:2], ln_bias[0, 1:2], spm
    )
    blocks = gather_blocks(normed, n_mp)
    partials = [mlp(blocks[k], up, b_up, down, k) for k in range(n_mp)]
    added = scatter_blocks(partials, n_mp)
    own_labels = lax.dynamic_slice_in_dim(labcol, m * spm, spm)
    return finish(added, residual, b_down, own_labels)


def solution(mesh):
    in_specs = (
        P(("dp", "mp"), None, None),
        P(),
        P(("dp", "mp"), None),
        P(),
        P(),
        P(),
        P(),
        P(None, None, "dp", "mp"),
        P(None, None, "mp"),
        P(None, "mp", "dp"),
        P(),
        P(None, "dp", "mp"),
        P(None, "mp"),
        P(None, "mp", "dp"),
        P(),
    )
    out_specs = P(("dp", "mp"), None)
    return jax.shard_map(
        per_device, mesh=mesh, in_specs=in_specs, out_specs=out_specs, check_vma=False
    )
```

```python
import functools
import math

import jax
import jax.numpy as jnp
from jax import lax
from jax.experimental import pallas as pl
from jax.experimental.pallas import tpu as pltpu
from jax.sharding import PartitionSpec as P


HEAD = 80
LANES = 128
BF = jnp.bfloat16
F32 = jnp.float32
NT = (((1,), (1,)), ((), ()))


def cost(flops, moved):
    return pl.CostEstimate(flops=int(flops), bytes_accessed=int(moved), transcendentals=0)


def params(mib=48):
    return pltpu.CompilerParams(vmem_limit_bytes=mib * 1024 * 1024)


def embed_kernel(place_ref, keep_ref, patches_ref, position_ref, *refs):
    out_refs, token_ref = refs[:-1], refs[-1]
    per, patch_count, _ = patches_ref.shape
    row = keep_ref[0].astype(F32)
    tokens = row.shape[1]
    kept = jnp.broadcast_to(row, (tokens, tokens)).T
    reps = (patch_count + tokens - 1) // tokens
    wide = jnp.concatenate([kept] * reps, axis=1)[:, :patch_count]
    lane = lax.broadcasted_iota(jnp.int32, (tokens, patch_count), 1).astype(F32)
    onehot = jnp.where(wide == lane, 1.0, 0.0).astype(BF)
    each = tokens // per
    placed = jnp.dot(onehot, position_ref[...], preferred_element_type=F32)
    picked = jnp.concatenate(
        [
            jnp.dot(onehot[i * each : (i + 1) * each], patches_ref[i], preferred_element_type=F32)
            for i in range(per)
        ],
        axis=0,
    )
    token_ref[...] = (picked + placed).T.astype(BF).reshape(token_ref.shape)
    for k, ref in enumerate(out_refs):
        ref[...] = token_ref[jnp.bitwise_xor(place_ref[0], k)]


def embed(place, patches, position, keep, n_mp):
    images, patch_count, width = patches.shape
    keep_most = keep.shape[1]
    per = max(1, min(images, LANES // keep_most))
    steps = images // per
    tokens = per * keep_most
    return pl.pallas_call(
        embed_kernel,
        grid=(steps,),
        in_specs=[
            pl.BlockSpec(memory_space=pltpu.SMEM),
            pl.BlockSpec((1, 1, tokens), lambda i: (i, 0, 0)),
            pl.BlockSpec((per, patch_count, width), lambda i: (i, 0, 0)),
            pl.BlockSpec((patch_count, width), lambda i: (0, 0)),
        ],
        out_specs=[pl.BlockSpec((width // n_mp, tokens), lambda i: (0, i))] * n_mp,
        out_shape=[jax.ShapeDtypeStruct((width // n_mp, images * keep_most), BF)] * n_mp,
        scratch_shapes=[pltpu.VMEM((n_mp, width // n_mp, tokens), BF)],
        compiler_params=params(24),
        cost_estimate=cost(4e9, patches.size * 2),
        name="embed",
    )(place, keep.reshape(steps, 1, tokens), patches, position)


def pack_kernel(fold, slot_rows, group, n_src, place_ref, target_ref, *refs):
    feat_refs, out_refs = refs[:n_src], refs[n_src:]
    width, tokens = feat_refs[0].shape
    d = place_ref[1]
    piece = slot_rows // fold
    for g in range(0, len(out_refs), group):
        row = jnp.concatenate(
            [
                lax.broadcasted_iota(jnp.int32, (slot_rows, tokens), 0)
                + jnp.bitwise_xor(d, g + b) * slot_rows
                for b in range(group)
            ],
            axis=0,
        )
        total = jnp.zeros((group * slot_rows, width), F32)
        for j in range(n_src):
            at = jnp.bitwise_xor(place_ref[0], j)
            onehot = jnp.where(row == target_ref[at], 1.0, 0.0).astype(BF)
            total = total + lax.dot_general(onehot, feat_refs[j][...], NT, preferred_element_type=F32)
        for b in range(group):
            start = b * slot_rows
            chunks = [total[start + f * piece : start + (f + 1) * piece] for f in range(fold)]
            out_refs[g + b][...] = jnp.concatenate(chunks, axis=1).astype(BF)


def pack(place, featured, target, slots, slot_rows, fold):
    width, tokens = featured[0].shape
    smem = pl.BlockSpec(memory_space=pltpu.SMEM)
    vmem = pl.BlockSpec(memory_space=pltpu.VMEM)
    return pl.pallas_call(
        functools.partial(pack_kernel, fold, slot_rows, min(4, slots), len(featured)),
        in_specs=[smem] + [vmem] * (1 + len(featured)),
        out_specs=[vmem] * slots,
        out_shape=[jax.ShapeDtypeStruct((slot_rows // fold, fold * width), BF)] * slots,
        compiler_params=params(24),
        cost_estimate=cost(4e9, width * tokens * 8),
        name="pack",
    )(place, target, *featured)


def unfold(values, fold):
    width = values.shape[2] // fold
    values = values.astype(F32)
    pieces = [
        values[s, :, f * width : (f + 1) * width] for s in range(values.shape[0]) for f in range(fold)
    ]
    return jnp.concatenate(pieces, axis=0)


def fetch_start(groups, block, spm, buf_ref, sem_ref):
    for k, pieces in enumerate(groups):
        per = pieces[0].shape[0] // spm
        for i, piece in enumerate(pieces):

            def start(piece=piece, i=i, k=k):
                at = pl.ds((block - i * per) * spm, spm)
                pltpu.make_async_copy(piece.at[at], buf_ref.at[k], sem_ref.at[k]).start()

            here = len(pieces) == 1 or jnp.logical_and(block >= i * per, block < (i + 1) * per)
            if isinstance(block, int):
                if i * per <= block < (i + 1) * per:
                    start()
            elif here is True:
                start()
            else:
                pl.when(here)(start)


def fetch_wait(groups, spm, buf_ref, sem_ref):
    for k, pieces in enumerate(groups):
        pltpu.make_async_copy(pieces[0].at[pl.ds(0, spm)], buf_ref.at[k], sem_ref.at[k]).wait()


def cut(refs, counts):
    groups, at = [], 0
    for count in counts:
        groups.append(refs[at : at + count])
        at += count
    return groups, refs[at:]


def owner_block(place_ref, dest, spm):
    return jnp.bitwise_xor(jnp.bitwise_xor(place_ref[0], dest), place_ref[1] // spm)


def attend_block(block, gathered, me, refs, hc, spm):
    weight_ref, bias_ref, gain_ref, shift_ref, labrow, labcol, norm_ref = refs
    n_mp = len(gathered)
    _, width = gathered[0].shape
    full = width * n_mp
    mean = sum(jnp.sum(b, axis=1, keepdims=True) for b in gathered) * (1.0 / full)
    gathered = [b - mean for b in gathered]
    spread = sum(jnp.sum(b * b, axis=1, keepdims=True) for b in gathered) * (1.0 / full)
    scale = lax.rsqrt(spread + 1e-06)
    for k in range(n_mp):
        which = jnp.bitwise_xor(me, k)
        norm_ref[which] = (gathered[k] * scale * gain_ref[which] + shift_ref[which]).astype(BF)
    normed = jnp.concatenate([norm_ref[j] for j in range(n_mp)], axis=1)
    start = hc // LANES * LANES
    lead = hc - start
    qkv = jnp.dot(normed, weight_ref[:, start:], preferred_element_type=F32)
    query = qkv[:, lead : lead + hc] + bias_ref[:, :hc]
    query = (query * (1.0 / math.sqrt(HEAD))).astype(BF)
    key = (qkv[:, lead + hc : lead + 2 * hc] + bias_ref[:, hc : 2 * hc]).astype(BF)
    value = (qkv[:, lead + 2 * hc :] + bias_ref[:, 2 * hc :]).astype(BF)
    slot_rows = labcol.shape[1]
    heads = hc // HEAD
    lane_head = lax.broadcasted_iota(jnp.int32, (slot_rows, hc), 1) // HEAD
    results = []
    for s in range(spm):
        at = slice(s * slot_rows, (s + 1) * slot_rows)
        q, kk, v = query[at], key[at], value[at]
        zero = jnp.zeros_like(q)
        stacked = jnp.concatenate([jnp.where(lane_head == h, q, zero) for h in range(heads)], axis=0)
        scores = lax.dot_general(stacked, kk, NT, preferred_element_type=F32)
        same = labcol[block * spm + s] == labrow[block * spm + s]
        outs = jnp.zeros((slot_rows, hc), F32)
        for h in range(heads):
            sh = jnp.where(same, scores[h * slot_rows : (h + 1) * slot_rows], -jnp.inf)
            e = jnp.exp(sh - jnp.max(sh, axis=1, keepdims=True))
            prob = (e * (1.0 / jnp.sum(e, axis=1, keepdims=True))).astype(BF)
            outs = jnp.where(lane_head == h, jnp.dot(prob, v, preferred_element_type=F32), outs)
        results.append(outs)
    return jnp.concatenate(results, axis=1).astype(BF)


def attend_kernel(counts, blocks, last, spm, fold, hc, place_ref, *refs):
    n_mp = len(counts)
    groups, refs = cut(refs, counts)
    operands, refs = list(refs[:6]), refs[6:]
    prior, refs = (refs[0], refs[1:]) if last else (None, refs)
    outs = n_mp if last else 1
    out_refs, (norm_ref, buf_ref, sem_ref, mine_ref) = refs[:outs], refs[outs:]
    for i, block in enumerate(blocks):
        fetch_start(groups, block, spm, buf_ref.at[i], sem_ref.at[i])
    for i, block in enumerate(blocks):
        fetch_wait(groups, spm, buf_ref.at[i], sem_ref.at[i])
        gathered = [unfold(buf_ref[i, k], fold) for k in range(n_mp)]
        value = attend_block(block, gathered, place_ref[0], operands + [norm_ref], hc, spm)
        if last:
            mine_ref[i] = value
        else:
            out_refs[0][i] = value
    if last:
        for k in range(n_mp):
            block = owner_block(place_ref, k, spm)
            before = prior[jnp.minimum(block, blocks[0] - 1)]
            later = mine_ref[jnp.maximum(block - blocks[0], 0)]
            out_refs[k][...] = jnp.where(block < blocks[0], before, later)


def attend(place, gathered, blocks, prior, fold, hc, operands, spm):
    n_mp = len(gathered)
    _, piece, lanes = gathered[0][0].shape
    slot_rows = operands[4].shape[2]
    flat = sum(gathered, [])
    smem = pl.BlockSpec(memory_space=pltpu.SMEM)
    vmem = pl.BlockSpec(memory_space=pltpu.VMEM)
    last = prior is not None
    shape = (slot_rows, spm * hc)
    if last:
        out_shape = [jax.ShapeDtypeStruct(shape, BF)] * n_mp
    else:
        out_shape = [jax.ShapeDtypeStruct((len(blocks), *shape), BF)]
    return pl.pallas_call(
        functools.partial(
            attend_kernel, [len(g) for g in gathered], blocks, last, spm, fold, hc
        ),
        in_specs=[smem]
        + [pl.BlockSpec(memory_space=pltpu.HBM)] * len(flat)
        + [vmem] * (len(operands) + last),
        out_specs=[vmem] * len(out_shape),
        scratch_shapes=[
            pltpu.VMEM((n_mp, spm * slot_rows, lanes // fold), BF),
            pltpu.VMEM((len(blocks), n_mp, spm, piece, lanes), BF),
            pltpu.SemaphoreType.DMA((len(blocks), n_mp)),
            pltpu.VMEM((len(blocks), *shape), BF),
        ],
        out_shape=out_shape,
        compiler_params=params(24),
        cost_estimate=cost(len(blocks) * 4e9, operands[0].size * 4),
        name="attend",
    )(place, *flat, *operands, *([prior] if last else []))


def own_kernel(counts, spm, fold, place_ref, *refs):
    n_mp = len(counts)
    groups, (bias_ref, out_ref, buf_ref, sem_ref) = cut(refs, counts)
    fetch_start(groups, owner_block(place_ref, 0, spm), spm, buf_ref, sem_ref)
    fetch_wait(groups, spm, buf_ref, sem_ref)
    blocks = [unfold(buf_ref[k], fold) for k in range(n_mp)]
    ordered = []
    for j in range(n_mp):
        value = blocks[0]
        for k in range(1, n_mp):
            value = jnp.where(jnp.bitwise_xor(place_ref[0], k) == j, blocks[k], value)
        ordered.append(value)
    out_ref[...] = jnp.concatenate(ordered, axis=1) + bias_ref[...]


def own_rows(place, gathered, fold, bias, spm):
    n_mp = len(gathered)
    _, piece, lanes = gathered[0][0].shape
    features = sum(gathered, [])
    vmem = pl.BlockSpec(memory_space=pltpu.VMEM)
    return pl.pallas_call(
        functools.partial(own_kernel, [len(g) for g in gathered], spm, fold),
        in_specs=[pl.BlockSpec(memory_space=pltpu.SMEM)]
        + [pl.BlockSpec(memory_space=pltpu.HBM)] * len(features)
        + [vmem],
        out_specs=vmem,
        out_shape=jax.ShapeDtypeStruct((spm * piece * fold, bias.shape[1]), F32),
        scratch_shapes=[
            pltpu.VMEM((n_mp, spm, piece, lanes), BF),
            pltpu.SemaphoreType.DMA((n_mp,)),
        ],
        compiler_params=params(16),
        cost_estimate=cost(1e9, 4 * bias.size * piece),
        name="own",
    )(place, *features, bias)


def project_kernel(out_counts, spm, hc, place_ref, base_ref, *refs):
    n_mp = len(out_counts)
    att_refs, at = refs[:n_mp], n_mp
    own_ref, at = refs[at], at + 1
    half = own_ref.shape[0] // 2
    core = place_ref[1] % 2
    mine, mate = None, None
    for k, count in enumerate(out_counts):
        left = jnp.concatenate([att_refs[k][:, s * hc : (s + 1) * hc] for s in range(spm)], axis=0)
        if k == 0:
            pair = [
                [own_ref[pl.ds(pl.multiple_of(c * half, 128), half)]] for c in (core, 1 - core)
            ]
        else:
            pair = [[r[...] for r in refs[at : at + count]], [r[...] for r in refs[at + count : at + 2 * count]]]
            at += 2 * count
        sums = [
            jnp.concatenate(
                [lax.dot_general(left, w, NT, preferred_element_type=F32) for w in ws], axis=1
            )
            for ws in pair
        ]
        mine, mate = (sums[0], sums[1]) if mine is None else (mine + sums[0], mate + sums[1])
    total = jnp.concatenate(
        [jnp.where(core == 0, mine, mate), jnp.where(core == 0, mate, mine)], axis=1
    )
    gain_ref, shift_ref, res_ref, out_ref = refs[at:]
    value = base_ref[...] + total
    res_ref[...] = value
    mean = jnp.mean(value, axis=1, keepdims=True)
    value = value - mean
    spread = jnp.mean(value * value, axis=1, keepdims=True)
    out_ref[...] = (value * lax.rsqrt(spread + 1e-06) * gain_ref[...] + shift_ref[...]).astype(BF)


def project(place, base, hc, attended, out_weights, gain, shift, spm):
    n_mp = len(attended)
    weights = sum([sum(w, []) for w in out_weights], [])
    vmem = pl.BlockSpec(memory_space=pltpu.VMEM)
    return pl.pallas_call(
        functools.partial(project_kernel, [len(w[0]) for w in out_weights], spm, hc),
        in_specs=[pl.BlockSpec(memory_space=pltpu.SMEM)] + [vmem] * (n_mp + len(weights) + 3),
        out_specs=[vmem] * 2,
        out_shape=[jax.ShapeDtypeStruct(base.shape, F32), jax.ShapeDtypeStruct(base.shape, BF)],
        compiler_params=params(20),
        cost_estimate=cost(3e9, 16 * base.size),
        name="project",
    )(place, base, *attended, *weights, gain, shift)


def mlp_kernel(count, *refs):
    in_refs, (up_ref, bias_ref, down_ref), out_refs = refs[:count], refs[count : count + 3], refs[count + 4 :]
    rows = jnp.concatenate([r[...] for r in in_refs], axis=0)
    hidden_width = up_ref.shape[1]
    step = 256 if hidden_width % 256 == 0 else LANES
    hidden = []
    for c in range(0, hidden_width, step):
        at = slice(c, c + step)
        up = jnp.dot(rows, up_ref[:, at], preferred_element_type=F32) + bias_ref[:, at]
        hidden.append((0.5 * up * (1.0 + lax.erf(up * math.sqrt(0.5)))).astype(BF))
    hidden = jnp.concatenate(hidden, axis=1)
    each, width = out_refs[0].shape
    for c in range(0, width, 256):
        part = lax.dot_general(hidden, down_ref[c : c + 256], NT, preferred_element_type=F32)
        for i, ref in enumerate(out_refs):
            ref[:, c : c + 256] = part[i * each : (i + 1) * each].astype(BF)


def mlp(rows, outs, up, bias, down, after):
    width = down.shape[0]
    total = sum(r.shape[0] for r in rows)
    vmem = pl.BlockSpec(memory_space=pltpu.VMEM)
    return pl.pallas_call(
        functools.partial(mlp_kernel, len(rows)),
        in_specs=[vmem] * (len(rows) + 3) + [pl.BlockSpec(memory_space=pl.ANY)],
        out_specs=[vmem] * outs,
        out_shape=[jax.ShapeDtypeStruct((total // outs, width), BF)] * outs,
        compiler_params=params(20),
        cost_estimate=cost(total * up.size * 4, up.size * 4),
    )(*rows, up, bias, down, after)


def finish_kernel(adds, pieces, spm, place_ref, *refs):
    add_refs, (res_ref, bias_ref, lab_ref, out_ref) = refs[:adds], refs[adds:]
    each = res_ref.shape[0] // pieces
    labels = lab_ref[...].reshape(res_ref.shape[0], 1)
    turn = place_ref[1] % spm
    for s in range(pieces):
        at = slice(s * each, (s + 1) * each)
        value = res_ref[at] + bias_ref[...]
        for i in range(s, adds, pieces):
            value = value + add_refs[i][...].astype(F32)
        value = jnp.where(labels[at] >= 0, value, 0.0).astype(BF)
        out_ref[pl.ds(pl.multiple_of(jnp.bitwise_xor(turn, s) * each, 16), each)] = value


def finish(place, added, pieces, residual, bias, labels, spm):
    smem = pl.BlockSpec(memory_space=pltpu.SMEM)
    vmem = pl.BlockSpec(memory_space=pltpu.VMEM)
    return pl.pallas_call(
        functools.partial(finish_kernel, len(added), pieces, spm),
        in_specs=[smem] + [vmem] * (len(added) + 3),
        out_specs=vmem,
        out_shape=jax.ShapeDtypeStruct(residual.shape, BF),
        compiler_params=params(16),
        cost_estimate=cost(1e9, residual.size * 8),
        name="finish",
    )(place, *added, residual, bias, labels)


def hop(value, k, n):
    return lax.ppermute(value, "mp", [(i, i ^ k) for i in range(n)])


def after(value, *others):
    return lax.optimization_barrier((value, *others))[0]


def gather_blocks(value, n):
    if n != 4:
        return [[value]] + [[hop(value, k, n)] for k in range(1, n)]
    half = value.shape[0] // 2
    x = hop(value, 1, n)
    y = hop(value, 2, n)
    far = [hop(x[:half], 2, n), hop(y[half:], 1, n)]
    return [[value], [x], [y], far]


def plus(a, b):
    return (a.astype(F32) + b.astype(F32)).astype(BF)


def scatter_blocks(partials, n):
    own = list(partials[0])
    if n != 4 or len(own) != 2:
        for k in range(1, n):
            own += [hop(p, k, n) for p in partials[k]]
        return own
    far, x, y = partials[3], partials[1], partials[2]
    x0, y1 = hop(x[0], 1, n), hop(y[1], 2, n)
    first, second = hop(far[0], 1, n), hop(far[1], 2, n)
    y0, x1 = hop(plus(y[0], first), 2, n), hop(plus(x[1], second), 1, n)
    return own + [x0, x1, y0, y1]


def per_device(
    patches,
    position,
    keep,
    counts,
    offsets,
    ln_gain,
    ln_bias,
    w_qkv,
    b_qkv,
    w_o,
    b_o,
    w_up,
    b_up,
    w_down,
    b_down,
):
    local_images, _, width = patches.shape
    keep_most = keep.shape[1]
    n_dp, n_mp = lax.axis_size("dp"), lax.axis_size("mp")
    d, m = lax.axis_index("dp"), lax.axis_index("mp")
    images_here = local_images * n_mp
    per_slot = (images_here + n_dp - 1) // n_dp
    slot_rows = max(keep_most + 16, per_slot * keep_most * 5 // 8)
    pack_rows = slot_rows * n_dp
    spm = n_dp // n_mp
    feat = width // n_mp
    hc = w_qkv.shape[3]
    place = jnp.stack([m, d]).astype(jnp.int32)

    tokens = embed(place, patches, position, keep, n_mp)
    featured = [tokens[0]] + [hop(tokens[k], k, n_mp) for k in range(1, n_mp)]

    w_qkv, w_o = after(w_qkv, tokens[0]), after(w_o, tokens[0])
    mixed = jnp.concatenate([w_o[0].T, w_qkv[0, 0], w_qkv[0, 1], w_qkv[0, 2]], axis=1)
    mixed = lax.all_gather(mixed, "dp", axis=0, tiled=True)
    own = mixed[:, :hc]
    part = lax.dynamic_slice_in_dim(own, (d % 2) * (width // 2), width // 2)
    mate = [(i, i ^ 1) for i in range(n_dp)]
    out_weights = [[[own]]]
    for pieces in gather_blocks(part, n_mp)[1:]:
        out_weights.append([pieces, [lax.ppermute(p, "dp", mate) for p in pieces]])

    first_image = d * images_here
    group_counts = lax.dynamic_slice_in_dim(counts, first_image, images_here)
    group_offsets = lax.dynamic_slice_in_dim(offsets, first_image, images_here)
    shard_index = group_offsets // pack_rows
    base_row = shard_index * slot_rows + group_offsets - shard_index * pack_rows - d * slot_rows
    spot = jnp.arange(keep_most, dtype=jnp.int32)
    target = jnp.where(
        spot[None, :] < group_counts[:, None], base_row[:, None] + spot[None, :], pack_rows
    ).reshape(n_mp, 1, local_images * keep_most)
    fold = 2
    packed = pack(place, featured, target, n_dp, slot_rows, fold)
    half = n_dp // 2
    moved = [packed[0]]
    for i in range(1, n_dp):
        moved.append(lax.ppermute(packed[i], "dp", [(j, j ^ i) for j in range(n_dp)]))
    near = jnp.stack(moved[:half])
    far = jnp.stack(moved[half:])
    halves = [near, far]
    up = lax.all_gather(w_up[0], "dp", axis=0, tiled=True)
    down = lax.all_gather(w_down[0].T, "dp", axis=0, tiled=True)

    image_ids = jnp.arange(counts.shape[0], dtype=jnp.int32)
    slots = jnp.bitwise_xor(jnp.arange(n_dp, dtype=jnp.int32), d)
    packed_rows = d * pack_rows + slots[:, None] * slot_rows + jnp.arange(slot_rows, dtype=jnp.int32)
    packed_rows = packed_rows.reshape(pack_rows)
    inside = (packed_rows[:, None] >= offsets[None, :]) & (
        packed_rows[:, None] < (offsets + counts)[None, :]
    )
    labels = jnp.max(jnp.where(inside, image_ids[None, :] + 1, 0), axis=1) - 1
    labrow = labels.reshape(n_dp, 1, slot_rows)
    labcol = labels.reshape(n_dp, slot_rows, 1)

    moved = [gather_blocks(h, n_mp) for h in halves]
    gathered = [sum(pieces, []) for pieces in zip(*moved)]
    gain = ln_gain[0, 0].reshape(n_mp, 1, feat)
    shift = ln_bias[0, 0].reshape(n_mp, 1, feat)
    bias = b_qkv[0].reshape(1, 3 * hc)
    operands = (mixed, bias, gain, shift, labrow, labcol)
    count = n_dp // spm
    ahead = list(range(count // 2))
    prior = attend(place, moved[0], ahead, None, fold, hc, operands, spm)[0]
    attended = attend(
        place, gathered, list(range(count // 2, count)), prior, fold, hc, operands, spm
    )
    attended = [attended[0]] + [hop(attended[k], k, n_mp) for k in range(1, n_mp)]
    base = own_rows(place, gathered, fold, b_o, spm)
    residual, normed = project(
        place, base, hc, attended, out_weights, ln_gain[0, 1:2], ln_bias[0, 1:2], spm
    )
    blocks = gather_blocks(normed, n_mp)
    partials = [None] * n_mp
    last = normed
    groups = [[0], [2, 1], [3]] if n_mp == 4 else [[k] for k in range(n_mp)]
    for group in groups:
        outs = mlp(sum([blocks[k] for k in group], []), 2 * len(group), up, b_up, down, last)
        last = outs[0]
        for i, k in enumerate(group):
            partials[k] = outs[2 * i : 2 * i + 2]
    added = scatter_blocks(partials, n_mp)
    own_labels = lax.dynamic_slice_in_dim(labcol, jnp.bitwise_xor(m, d // spm) * spm, spm)
    return finish(place, added, 2, residual, b_down, own_labels, spm)


def solution(mesh):
    in_specs = (
        P(("dp", "mp"), None, None),
        P(),
        P(("dp", "mp"), None),
        P(),
        P(),
        P(),
        P(),
        P(None, None, "dp", "mp"),
        P(None, None, "mp"),
        P(None, "mp", "dp"),
        P(),
        P(None, "dp", "mp"),
        P(None, "mp"),
        P(None, "mp", "dp"),
        P(),
    )
    out_specs = P(("dp", "mp"), None)

    return jax.shard_map(
        per_device, mesh=mesh, in_specs=in_specs, out_specs=out_specs, check_vma=False
    )
```

```python
import functools
import math

import jax
import jax.numpy as jnp
from jax import lax
from jax.experimental import pallas as pl
from jax.experimental.pallas import tpu as pltpu
from jax.sharding import PartitionSpec as P


HEAD = 80
LANES = 128
BF = jnp.bfloat16
F32 = jnp.float32
NT = (((1,), (1,)), ((), ()))


def cost(flops, moved):
    return pl.CostEstimate(flops=int(flops), bytes_accessed=int(moved), transcendentals=0)


def params(mib=48):
    return pltpu.CompilerParams(vmem_limit_bytes=mib * 1024 * 1024)


def embed_kernel(place_ref, keep_ref, patches_ref, position_ref, *refs):
    out_refs, token_ref = refs[:-1], refs[-1]
    per, patch_count, _ = patches_ref.shape
    row = keep_ref[0].astype(F32)
    tokens = row.shape[1]
    kept = jnp.broadcast_to(row, (tokens, tokens)).T
    reps = (patch_count + tokens - 1) // tokens
    wide = jnp.concatenate([kept] * reps, axis=1)[:, :patch_count]
    lane = lax.broadcasted_iota(jnp.int32, (tokens, patch_count), 1).astype(F32)
    onehot = jnp.where(wide == lane, 1.0, 0.0).astype(BF)
    each = tokens // per
    placed = jnp.dot(onehot, position_ref[...], preferred_element_type=F32)
    picked = jnp.concatenate(
        [
            jnp.dot(onehot[i * each : (i + 1) * each], patches_ref[i], preferred_element_type=F32)
            for i in range(per)
        ],
        axis=0,
    )
    token_ref[...] = (picked + placed).T.astype(BF).reshape(token_ref.shape)
    for k, ref in enumerate(out_refs):
        ref[...] = token_ref[jnp.bitwise_xor(place_ref[0], k)]


def embed(place, patches, position, keep, n_mp):
    images, patch_count, width = patches.shape
    keep_most = keep.shape[1]
    per = max(1, min(images, LANES // keep_most))
    steps = images // per
    tokens = per * keep_most
    return pl.pallas_call(
        embed_kernel,
        grid=(steps,),
        in_specs=[
            pl.BlockSpec(memory_space=pltpu.SMEM),
            pl.BlockSpec((1, 1, tokens), lambda i: (i, 0, 0)),
            pl.BlockSpec((per, patch_count, width), lambda i: (i, 0, 0)),
            pl.BlockSpec((patch_count, width), lambda i: (0, 0)),
        ],
        out_specs=[pl.BlockSpec((width // n_mp, tokens), lambda i: (0, i))] * n_mp,
        out_shape=[jax.ShapeDtypeStruct((width // n_mp, images * keep_most), BF)] * n_mp,
        scratch_shapes=[pltpu.VMEM((n_mp, width // n_mp, tokens), BF)],
        compiler_params=params(60),
        cost_estimate=cost(4e9, patches.size * 2),
        name="embed",
    )(place, keep.reshape(steps, 1, tokens), patches, position)


def pack_kernel(fold, slot_rows, group, n_src, place_ref, target_ref, *refs):
    feat_refs, out_refs = refs[:n_src], refs[n_src:]
    width, tokens = feat_refs[0].shape
    d = place_ref[1]
    piece = slot_rows // fold
    for g in range(0, len(out_refs), group):
        row = jnp.concatenate(
            [
                lax.broadcasted_iota(jnp.int32, (slot_rows, tokens), 0)
                + jnp.bitwise_xor(d, g + b) * slot_rows
                for b in range(group)
            ],
            axis=0,
        )
        total = jnp.zeros((group * slot_rows, width), F32)
        for j in range(n_src):
            at = jnp.bitwise_xor(place_ref[0], j)
            onehot = jnp.where(row == target_ref[at], 1.0, 0.0).astype(BF)
            total = total + lax.dot_general(onehot, feat_refs[j][...], NT, preferred_element_type=F32)
        for b in range(group):
            start = b * slot_rows
            chunks = [total[start + f * piece : start + (f + 1) * piece] for f in range(fold)]
            out_refs[g + b][...] = jnp.concatenate(chunks, axis=1).astype(BF)


def pack(place, featured, target, slots, slot_rows, fold):
    width, tokens = featured[0].shape
    smem = pl.BlockSpec(memory_space=pltpu.SMEM)
    vmem = pl.BlockSpec(memory_space=pltpu.VMEM)
    return pl.pallas_call(
        functools.partial(pack_kernel, fold, slot_rows, min(4, slots), len(featured)),
        in_specs=[smem] + [vmem] * (1 + len(featured)),
        out_specs=[vmem] * slots,
        out_shape=[jax.ShapeDtypeStruct((slot_rows // fold, fold * width), BF)] * slots,
        compiler_params=params(24),
        cost_estimate=cost(4e9, width * tokens * 8),
        name="pack",
    )(place, target, *featured)


def unfold(values, fold):
    width = values.shape[2] // fold
    values = values.astype(F32)
    pieces = [
        values[s, :, f * width : (f + 1) * width] for s in range(values.shape[0]) for f in range(fold)
    ]
    return jnp.concatenate(pieces, axis=0)


def fetch_start(groups, block, spm, buf_ref, sem_ref):
    for k, pieces in enumerate(groups):
        low = 0
        for piece in pieces:
            high = low + piece.shape[0] // spm

            def start(piece=piece, k=k, low=low):
                at = pl.ds((block - low) * spm, spm)
                pltpu.make_async_copy(piece.at[at], buf_ref.at[k], sem_ref.at[k]).start()

            if isinstance(block, int):
                if low <= block < high:
                    start()
            elif len(pieces) == 1:
                start()
            else:
                pl.when(jnp.logical_and(block >= low, block < high))(start)
            low = high


def fetch_wait(groups, spm, buf_ref, sem_ref):
    for k, pieces in enumerate(groups):
        pltpu.make_async_copy(pieces[0].at[pl.ds(0, spm)], buf_ref.at[k], sem_ref.at[k]).wait()


def cut(refs, counts):
    groups, at = [], 0
    for count in counts:
        groups.append(refs[at : at + count])
        at += count
    return groups, refs[at:]


def owner_block(place_ref, dest, spm):
    return jnp.bitwise_xor(jnp.bitwise_xor(place_ref[0], dest), place_ref[1] // spm)


def attend_block(block, gathered, me, refs, hc, spm):
    weight_ref, bias_ref, gain_ref, shift_ref, labrow, labcol, norm_ref = refs
    n_mp = len(gathered)
    _, width = gathered[0].shape
    full = width * n_mp
    mean = sum(jnp.sum(b, axis=1, keepdims=True) for b in gathered) * (1.0 / full)
    gathered = [b - mean for b in gathered]
    spread = sum(jnp.sum(b * b, axis=1, keepdims=True) for b in gathered) * (1.0 / full)
    scale = lax.rsqrt(spread + 1e-06)
    for k in range(n_mp):
        which = jnp.bitwise_xor(me, k)
        norm_ref[which] = (gathered[k] * scale * gain_ref[which] + shift_ref[which]).astype(BF)
    normed = jnp.concatenate([norm_ref[j] for j in range(n_mp)], axis=1)
    start = hc // LANES * LANES
    lead = hc - start
    qkv = jnp.dot(normed, weight_ref[:, start:], preferred_element_type=F32)
    query = qkv[:, lead : lead + hc] + bias_ref[:, :hc]
    query = (query * (1.0 / math.sqrt(HEAD))).astype(BF)
    key = (qkv[:, lead + hc : lead + 2 * hc] + bias_ref[:, hc : 2 * hc]).astype(BF)
    value = (qkv[:, lead + 2 * hc :] + bias_ref[:, 2 * hc :]).astype(BF)
    slot_rows = labcol.shape[1]
    heads = hc // HEAD
    lane_head = lax.broadcasted_iota(jnp.int32, (slot_rows, hc), 1) // HEAD
    results = []
    for s in range(spm):
        at = slice(s * slot_rows, (s + 1) * slot_rows)
        q, kk, v = query[at], key[at], value[at]
        zero = jnp.zeros_like(q)
        stacked = jnp.concatenate([jnp.where(lane_head == h, q, zero) for h in range(heads)], axis=0)
        scores = lax.dot_general(stacked, kk, NT, preferred_element_type=F32)
        same = labcol[block * spm + s] == labrow[block * spm + s]
        outs = jnp.zeros((slot_rows, hc), F32)
        for h in range(heads):
            sh = jnp.where(same, scores[h * slot_rows : (h + 1) * slot_rows], -jnp.inf)
            e = jnp.exp(sh - jnp.max(sh, axis=1, keepdims=True))
            prob = (e * (1.0 / jnp.sum(e, axis=1, keepdims=True))).astype(BF)
            outs = jnp.where(lane_head == h, jnp.dot(prob, v, preferred_element_type=F32), outs)
        results.append(outs)
    return jnp.concatenate(results, axis=1).astype(BF)


def attend_kernel(counts, blocks, last, spm, fold, hc, place_ref, *refs):
    n_mp = len(counts)
    groups, refs = cut(refs, counts)
    operands, refs = list(refs[:6]), refs[6:]
    prior, refs = (refs[0], refs[1:]) if last else (None, refs)
    outs = n_mp if last else 1
    out_refs, (norm_ref, buf_ref, sem_ref, mine_ref) = refs[:outs], refs[outs:]
    for i, block in enumerate(blocks):
        fetch_start(groups, block, spm, buf_ref.at[i], sem_ref.at[i])
    for i, block in enumerate(blocks):
        fetch_wait(groups, spm, buf_ref.at[i], sem_ref.at[i])
        gathered = [unfold(buf_ref[i, k], fold) for k in range(n_mp)]
        value = attend_block(block, gathered, place_ref[0], operands + [norm_ref], hc, spm)
        if last:
            mine_ref[i] = value
        else:
            out_refs[0][i] = value
    if last:
        for k in range(n_mp):
            block = owner_block(place_ref, k, spm)
            before = prior[jnp.minimum(block, blocks[0] - 1)]
            later = mine_ref[jnp.maximum(block - blocks[0], 0)]
            out_refs[k][...] = jnp.where(block < blocks[0], before, later)


def attend(place, gathered, blocks, prior, fold, hc, operands, spm):
    n_mp = len(gathered)
    _, piece, lanes = gathered[0][0].shape
    slot_rows = operands[4].shape[2]
    flat = sum(gathered, [])
    smem = pl.BlockSpec(memory_space=pltpu.SMEM)
    vmem = pl.BlockSpec(memory_space=pltpu.VMEM)
    last = prior is not None
    shape = (slot_rows, spm * hc)
    if last:
        out_shape = [jax.ShapeDtypeStruct(shape, BF)] * n_mp
    else:
        out_shape = [jax.ShapeDtypeStruct((len(blocks), *shape), BF)]
    return pl.pallas_call(
        functools.partial(
            attend_kernel, [len(g) for g in gathered], blocks, last, spm, fold, hc
        ),
        in_specs=[smem]
        + [pl.BlockSpec(memory_space=pltpu.HBM)] * len(flat)
        + [vmem] * (len(operands) + last),
        out_specs=[vmem] * len(out_shape),
        scratch_shapes=[
            pltpu.VMEM((n_mp, spm * slot_rows, lanes // fold), BF),
            pltpu.VMEM((len(blocks), n_mp, spm, piece, lanes), BF),
            pltpu.SemaphoreType.DMA((len(blocks), n_mp)),
            pltpu.VMEM((len(blocks), *shape), BF),
        ],
        out_shape=out_shape,
        compiler_params=params(24),
        cost_estimate=cost(len(blocks) * 4e9, operands[0].size * 4),
        name="attend",
    )(place, *flat, *operands, *([prior] if last else []))


def own_kernel(counts, spm, fold, place_ref, *refs):
    n_mp = len(counts)
    groups, (bias_ref, out_ref, buf_ref, sem_ref) = cut(refs, counts)
    fetch_start(groups, owner_block(place_ref, 0, spm), spm, buf_ref, sem_ref)
    fetch_wait(groups, spm, buf_ref, sem_ref)
    blocks = [unfold(buf_ref[k], fold) for k in range(n_mp)]
    ordered = []
    for j in range(n_mp):
        value = blocks[0]
        for k in range(1, n_mp):
            value = jnp.where(jnp.bitwise_xor(place_ref[0], k) == j, blocks[k], value)
        ordered.append(value)
    out_ref[...] = jnp.concatenate(ordered, axis=1) + bias_ref[...]


def own_rows(place, gathered, fold, bias, spm):
    n_mp = len(gathered)
    _, piece, lanes = gathered[0][0].shape
    features = sum(gathered, [])
    vmem = pl.BlockSpec(memory_space=pltpu.VMEM)
    return pl.pallas_call(
        functools.partial(own_kernel, [len(g) for g in gathered], spm, fold),
        in_specs=[pl.BlockSpec(memory_space=pltpu.SMEM)]
        + [pl.BlockSpec(memory_space=pltpu.HBM)] * len(features)
        + [vmem],
        out_specs=vmem,
        out_shape=jax.ShapeDtypeStruct((spm * piece * fold, bias.shape[1]), F32),
        scratch_shapes=[
            pltpu.VMEM((n_mp, spm, piece, lanes), BF),
            pltpu.SemaphoreType.DMA((n_mp,)),
        ],
        compiler_params=params(16),
        cost_estimate=cost(1e9, 4 * bias.size * piece),
        name="own",
    )(place, *features, bias)


def project_kernel(out_counts, spm, hc, place_ref, base_ref, *refs):
    n_mp = len(out_counts)
    att_refs, at = refs[:n_mp], n_mp
    own_ref, at = refs[at], at + 1
    half = own_ref.shape[0] // 2
    core = place_ref[1] % 2
    mine, mate = None, None
    for k, count in enumerate(out_counts):
        left = jnp.concatenate([att_refs[k][:, s * hc : (s + 1) * hc] for s in range(spm)], axis=0)
        if k == 0:
            pair = [
                [own_ref[pl.ds(pl.multiple_of(c * half, 128), half)]] for c in (core, 1 - core)
            ]
        else:
            pair = [[r[...] for r in refs[at : at + count]], [r[...] for r in refs[at + count : at + 2 * count]]]
            at += 2 * count
        sums = [
            jnp.concatenate(
                [lax.dot_general(left, w, NT, preferred_element_type=F32) for w in ws], axis=1
            )
            for ws in pair
        ]
        mine, mate = (sums[0], sums[1]) if mine is None else (mine + sums[0], mate + sums[1])
    total = jnp.concatenate(
        [jnp.where(core == 0, mine, mate), jnp.where(core == 0, mate, mine)], axis=1
    )
    gain_ref, shift_ref, res_ref, *out_refs = refs[at:]
    value = base_ref[...] + total
    res_ref[...] = value
    mean = jnp.mean(value, axis=1, keepdims=True)
    value = value - mean
    spread = jnp.mean(value * value, axis=1, keepdims=True)
    value = (value * lax.rsqrt(spread + 1e-06) * gain_ref[...] + shift_ref[...]).astype(BF)
    each = out_refs[0].shape[0]
    for i, ref in enumerate(out_refs):
        ref[...] = value[i * each : (i + 1) * each]


def project(place, base, hc, attended, out_weights, gain, shift, spm):
    n_mp = len(attended)
    weights = sum([sum(w, []) for w in out_weights], [])
    vmem = pl.BlockSpec(memory_space=pltpu.VMEM)
    return pl.pallas_call(
        functools.partial(project_kernel, [len(w[0]) for w in out_weights], spm, hc),
        in_specs=[pl.BlockSpec(memory_space=pltpu.SMEM)] + [vmem] * (n_mp + len(weights) + 3),
        out_specs=[vmem] * 3,
        out_shape=[jax.ShapeDtypeStruct(base.shape, F32)]
        + [jax.ShapeDtypeStruct((base.shape[0] // 2, base.shape[1]), BF)] * 2,
        compiler_params=params(20),
        cost_estimate=cost(3e9, 16 * base.size),
        name="project",
    )(place, base, *attended, *weights, gain, shift)


def mlp_kernel(count, *refs):
    in_refs, (weight_ref, bias_ref), out_refs = refs[:count], refs[count : count + 2], refs[count + 3 :]
    rows = jnp.concatenate([r[...] for r in in_refs], axis=0)
    hidden_width = bias_ref.shape[1]
    step = 256 if hidden_width % 256 == 0 else LANES
    hidden = []
    for c in range(0, hidden_width, step):
        at = slice(c, c + step)
        up = jnp.dot(rows, weight_ref[:, at], preferred_element_type=F32) + bias_ref[:, at]
        hidden.append((0.5 * up * (1.0 + lax.erf(up * math.sqrt(0.5)))).astype(BF))
    hidden = jnp.concatenate(hidden, axis=1)
    each, width = out_refs[0].shape
    for c in range(0, width, 256):
        part = lax.dot_general(
            hidden, weight_ref[c : c + 256, hidden_width:], NT, preferred_element_type=F32
        )
        for i, ref in enumerate(out_refs):
            ref[:, c : c + 256] = part[i * each : (i + 1) * each].astype(BF)


def mlp(rows, outs, weight, bias, after):
    width = weight.shape[0]
    total = sum(r.shape[0] for r in rows)
    vmem = pl.BlockSpec(memory_space=pltpu.VMEM)
    return pl.pallas_call(
        functools.partial(mlp_kernel, len(rows)),
        in_specs=[vmem] * (len(rows) + 2) + [pl.BlockSpec(memory_space=pl.ANY)],
        out_specs=[vmem] * outs,
        out_shape=[jax.ShapeDtypeStruct((total // outs, width), BF)] * outs,
        compiler_params=params(20),
        cost_estimate=cost(total * weight.size * 2, weight.size * 2),
    )(*rows, weight, bias, after)


def finish_kernel(adds, pieces, spm, place_ref, *refs):
    add_refs, (res_ref, bias_ref, lab_ref, out_ref) = refs[:adds], refs[adds:]
    each = res_ref.shape[0] // pieces
    labels = lab_ref[...].reshape(res_ref.shape[0], 1)
    turn = place_ref[1] % spm
    for s in range(pieces):
        at = slice(s * each, (s + 1) * each)
        value = res_ref[at] + bias_ref[...]
        for i in range(s, adds, pieces):
            value = value + add_refs[i][...].astype(F32)
        value = jnp.where(labels[at] >= 0, value, 0.0).astype(BF)
        out_ref[pl.ds(pl.multiple_of(jnp.bitwise_xor(turn, s) * each, 16), each)] = value


def finish(place, added, pieces, residual, bias, labels, spm):
    smem = pl.BlockSpec(memory_space=pltpu.SMEM)
    vmem = pl.BlockSpec(memory_space=pltpu.VMEM)
    return pl.pallas_call(
        functools.partial(finish_kernel, len(added), pieces, spm),
        in_specs=[smem] + [vmem] * (len(added) + 3),
        out_specs=vmem,
        out_shape=jax.ShapeDtypeStruct(residual.shape, BF),
        compiler_params=params(16),
        cost_estimate=cost(1e9, residual.size * 8),
        name="finish",
    )(place, *added, residual, bias, labels)


def hop(value, k, n):
    return lax.ppermute(value, "mp", [(i, i ^ k) for i in range(n)])


def gather_blocks(values, n, direct=False):
    if n != 4:
        return [values] + [[hop(v, k, n) for v in values] for k in range(1, n)]
    x = [hop(v, 1, n) for v in values]
    y = [hop(v, 2, n) for v in values[::-1]][::-1]
    if direct:
        return [values, x, y, [hop(v, 3, n) for v in values]]
    half = values[0].shape[0] // 2
    top, bottom = (x[0], y[1]) if len(values) == 2 else (x[0][:half], y[0][half:])
    far = [hop(top, 2, n), hop(bottom, 1, n)]
    return [values, x, y, far]


def plus(a, b):
    return (a.astype(F32) + b.astype(F32)).astype(BF)


def scatter_blocks(partials, n):
    own = list(partials[0])
    if n != 4 or len(own) != 2:
        for k in range(1, n):
            own += [hop(p, k, n) for p in partials[k]]
        return own
    far, x, y = partials[3], partials[1], partials[2]
    x0, y1 = hop(x[0], 1, n), hop(y[1], 2, n)
    first, second = hop(far[0], 1, n), hop(far[1], 2, n)
    y0, x1 = hop(plus(y[0], first), 2, n), hop(plus(x[1], second), 1, n)
    return own + [x0, x1, y0, y1]


def per_device(
    patches,
    position,
    keep,
    counts,
    offsets,
    ln_gain,
    ln_bias,
    w_qkv,
    b_qkv,
    w_o,
    b_o,
    w_up,
    b_up,
    w_down,
    b_down,
):
    local_images, _, width = patches.shape
    keep_most = keep.shape[1]
    n_dp, n_mp = lax.axis_size("dp"), lax.axis_size("mp")
    d, m = lax.axis_index("dp"), lax.axis_index("mp")
    images_here = local_images * n_mp
    per_slot = (images_here + n_dp - 1) // n_dp
    slot_rows = max(keep_most + 16, per_slot * keep_most * 5 // 8)
    pack_rows = slot_rows * n_dp
    spm = n_dp // n_mp
    feat = width // n_mp
    hc = w_qkv.shape[3]
    place = jnp.stack([m, d]).astype(jnp.int32)

    mixed = jnp.concatenate([w_o[0].T, w_qkv[0, 0], w_qkv[0, 1], w_qkv[0, 2]], axis=1)
    mixed = lax.all_gather(mixed, "dp", axis=0, tiled=True)
    tokens = embed(place, patches, position, keep, n_mp)
    featured = [tokens[0]] + [hop(tokens[k], k, n_mp) for k in range(1, n_mp)]

    own = mixed[:, :hc]
    part = lax.dynamic_slice_in_dim(own, (d % 2) * (width // 2), width // 2)
    mate = [(i, i ^ 1) for i in range(n_dp)]
    out_weights = [[[own]]]
    for pieces in gather_blocks([part], n_mp)[1:]:
        out_weights.append([pieces, [lax.ppermute(p, "dp", mate) for p in pieces]])

    first_image = d * images_here
    group_counts = lax.dynamic_slice_in_dim(counts, first_image, images_here)
    group_offsets = lax.dynamic_slice_in_dim(offsets, first_image, images_here)
    shard_index = group_offsets // pack_rows
    base_row = shard_index * slot_rows + group_offsets - shard_index * pack_rows - d * slot_rows
    spot = jnp.arange(keep_most, dtype=jnp.int32)
    target = jnp.where(
        spot[None, :] < group_counts[:, None], base_row[:, None] + spot[None, :], pack_rows
    ).reshape(n_mp, 1, local_images * keep_most)
    fold = 2
    packed = pack(place, featured, target, n_dp, slot_rows, fold)
    half = n_dp // 2
    moved = [packed[0]]
    for i in range(1, n_dp):
        moved.append(lax.ppermute(packed[i], "dp", [(j, j ^ i) for j in range(n_dp)]))
    near = jnp.stack(moved[:half])
    far = jnp.stack(moved[half:])
    halves = [near, far]
    both = jnp.concatenate([w_up[0], w_down[0].T], axis=1)
    both = lax.all_gather(both, "dp", axis=0, tiled=True)

    image_ids = jnp.arange(counts.shape[0], dtype=jnp.int32)
    slots = jnp.bitwise_xor(jnp.arange(n_dp, dtype=jnp.int32), d)
    packed_rows = d * pack_rows + slots[:, None] * slot_rows + jnp.arange(slot_rows, dtype=jnp.int32)
    packed_rows = packed_rows.reshape(pack_rows)
    inside = (packed_rows[:, None] >= offsets[None, :]) & (
        packed_rows[:, None] < (offsets + counts)[None, :]
    )
    labels = jnp.max(jnp.where(inside, image_ids[None, :] + 1, 0), axis=1) - 1
    labrow = labels.reshape(n_dp, 1, slot_rows)
    labcol = labels.reshape(n_dp, slot_rows, 1)

    moved = [gather_blocks([h], n_mp, i == 1) for i, h in enumerate(halves)]
    gathered = [sum(pieces, []) for pieces in zip(*moved)]
    gain = ln_gain[0, 0].reshape(n_mp, 1, feat)
    shift = ln_bias[0, 0].reshape(n_mp, 1, feat)
    bias = b_qkv[0].reshape(1, 3 * hc)
    operands = (mixed, bias, gain, shift, labrow, labcol)
    count = n_dp // spm
    ahead = list(range(count // 2))
    prior = attend(place, moved[0], ahead, None, fold, hc, operands, spm)[0]
    attended = attend(
        place, gathered, list(range(count // 2, count)), prior, fold, hc, operands, spm
    )
    attended = [attended[0]] + [hop(attended[k], k, n_mp) for k in range(1, n_mp)]
    base = own_rows(place, gathered, fold, b_o, spm)
    residual, *normed = project(
        place, base, hc, attended, out_weights, ln_gain[0, 1:2], ln_bias[0, 1:2], spm
    )
    blocks = gather_blocks(normed, n_mp)
    partials = [None] * n_mp
    last = normed[0]
    groups = [[0], [2, 1], [3]] if n_mp == 4 else [[k] for k in range(n_mp)]
    for group in groups:
        outs = mlp(sum([blocks[k] for k in group], []), 2 * len(group), both, b_up, last)
        last = outs[0]
        for i, k in enumerate(group):
            partials[k] = outs[2 * i : 2 * i + 2]
    added = scatter_blocks(partials, n_mp)
    own_labels = lax.dynamic_slice_in_dim(labcol, jnp.bitwise_xor(m, d // spm) * spm, spm)
    return finish(place, added, 2, residual, b_down, own_labels, spm)


def solution(mesh):
    in_specs = (
        P(("dp", "mp"), None, None),
        P(),
        P(("dp", "mp"), None),
        P(),
        P(),
        P(),
        P(),
        P(None, None, "dp", "mp"),
        P(None, None, "mp"),
        P(None, "mp", "dp"),
        P(),
        P(None, "dp", "mp"),
        P(None, "mp"),
        P(None, "mp", "dp"),
        P(),
    )
    out_specs = P(("dp", "mp"), None)

    return jax.shard_map(
        per_device, mesh=mesh, in_specs=in_specs, out_specs=out_specs, check_vma=False
    )
```

```python
import functools
import math

import jax
import jax.numpy as jnp
from jax import lax
from jax.experimental import pallas as pl
from jax.experimental.pallas import tpu as pltpu
from jax.sharding import PartitionSpec as P


HEAD = 80
LANES = 128
BF = jnp.bfloat16
F32 = jnp.float32
NT = (((1,), (1,)), ((), ()))


def cost(flops, moved):
    return pl.CostEstimate(flops=int(flops), bytes_accessed=int(moved), transcendentals=0)


def params(mib=48):
    return pltpu.CompilerParams(vmem_limit_bytes=mib * 1024 * 1024)


def embed_kernel(place_ref, keep_ref, patches_ref, position_ref, *refs):
    out_refs, token_ref = refs[:-1], refs[-1]
    per, patch_count, _ = patches_ref.shape
    first = pl.program_id(0) * per
    row = jnp.concatenate([keep_ref[pl.ds(first + i, 1)] for i in range(per)], axis=1).astype(F32)
    tokens = row.shape[1]
    kept = jnp.broadcast_to(row, (tokens, tokens)).T
    reps = (patch_count + tokens - 1) // tokens
    wide = jnp.concatenate([kept] * reps, axis=1)[:, :patch_count]
    lane = lax.broadcasted_iota(jnp.int32, (tokens, patch_count), 1).astype(F32)
    onehot = jnp.where(wide == lane, 1.0, 0.0).astype(BF)
    each = tokens // per
    placed = jnp.dot(onehot, position_ref[...], preferred_element_type=F32)
    picked = jnp.concatenate(
        [
            jnp.dot(onehot[i * each : (i + 1) * each], patches_ref[i], preferred_element_type=F32)
            for i in range(per)
        ],
        axis=0,
    )
    token_ref[...] = (picked + placed).T.astype(BF).reshape(token_ref.shape)
    for k, ref in enumerate(out_refs):
        ref[...] = token_ref[jnp.bitwise_xor(place_ref[0], k)]


def embed(place, patches, position, keep, n_mp):
    images, patch_count, width = patches.shape
    keep_most = keep.shape[1]
    per = max(1, min(images, LANES // keep_most))
    steps = images // per
    tokens = per * keep_most
    return pl.pallas_call(
        embed_kernel,
        grid=(steps,),
        in_specs=[
            pl.BlockSpec(memory_space=pltpu.SMEM),
            pl.BlockSpec(keep.shape, lambda i: (0, 0)),
            pl.BlockSpec((per, patch_count, width), lambda i: (i, 0, 0)),
            pl.BlockSpec((patch_count, width), lambda i: (0, 0)),
        ],
        out_specs=[pl.BlockSpec((width // n_mp, tokens), lambda i: (0, i))] * n_mp,
        out_shape=[jax.ShapeDtypeStruct((width // n_mp, images * keep_most), BF)] * n_mp,
        scratch_shapes=[pltpu.VMEM((n_mp, width // n_mp, tokens), BF)],
        compiler_params=params(60),
        cost_estimate=cost(4e9, patches.size * 2),
        name="embed",
    )(place, keep, patches, position)


def join_kernel(qkv_ref, out_ref, joined_ref):
    joined_ref[...] = jnp.concatenate(
        [out_ref[...]] + [qkv_ref[t] for t in range(qkv_ref.shape[0])], axis=1
    )


def join(w_qkv, w_o):
    kinds, rows, width = w_qkv.shape
    vmem = pl.BlockSpec(memory_space=pltpu.VMEM)
    return pl.pallas_call(
        join_kernel,
        in_specs=[vmem] * 2,
        out_specs=vmem,
        out_shape=jax.ShapeDtypeStruct((rows, (kinds + 1) * width), BF),
        compiler_params=params(60),
        cost_estimate=cost(1e8, 4 * rows * kinds * width),
        name="join",
    )(w_qkv, w_o)


def pack_kernel(fold, slot_rows, group, n_src, place_ref, target_ref, *refs):
    feat_refs, out_refs = refs[:n_src], refs[n_src:]
    width, tokens = feat_refs[0].shape
    d = place_ref[1]
    piece = slot_rows // fold
    for g in range(0, len(out_refs), group):
        row = jnp.concatenate(
            [
                lax.broadcasted_iota(jnp.int32, (slot_rows, tokens), 0)
                + jnp.bitwise_xor(d, g + b) * slot_rows
                for b in range(group)
            ],
            axis=0,
        )
        total = jnp.zeros((group * slot_rows, width), F32)
        for j in range(n_src):
            at = jnp.bitwise_xor(place_ref[0], j)
            onehot = jnp.where(row == target_ref[at], 1.0, 0.0).astype(BF)
            total = total + lax.dot_general(onehot, feat_refs[j][...], NT, preferred_element_type=F32)
        for b in range(group):
            start = b * slot_rows
            chunks = [total[start + f * piece : start + (f + 1) * piece] for f in range(fold)]
            out_refs[g + b][...] = jnp.concatenate(chunks, axis=1).astype(BF)


def pack(place, featured, target, slots, slot_rows, fold):
    width, tokens = featured[0].shape
    smem = pl.BlockSpec(memory_space=pltpu.SMEM)
    vmem = pl.BlockSpec(memory_space=pltpu.VMEM)
    return pl.pallas_call(
        functools.partial(pack_kernel, fold, slot_rows, min(4, slots), len(featured)),
        in_specs=[smem] + [vmem] * (1 + len(featured)),
        out_specs=[vmem] * slots,
        out_shape=[jax.ShapeDtypeStruct((slot_rows // fold, fold * width), BF)] * slots,
        compiler_params=params(24),
        cost_estimate=cost(4e9, width * tokens * 8),
        name="pack",
    )(place, target, *featured)


def unfold(values, fold):
    width = values.shape[2] // fold
    values = values.astype(F32)
    pieces = [
        values[s, :, f * width : (f + 1) * width] for s in range(values.shape[0]) for f in range(fold)
    ]
    return jnp.concatenate(pieces, axis=0)


def fetch_start(groups, block, spm, buf_ref, sem_ref):
    for k, pieces in enumerate(groups):
        low = 0
        for piece in pieces:
            high = low + piece.shape[0] // spm

            def start(piece=piece, k=k, low=low):
                at = pl.ds((block - low) * spm, spm)
                pltpu.make_async_copy(piece.at[at], buf_ref.at[k], sem_ref.at[k]).start()

            if isinstance(block, int):
                if low <= block < high:
                    start()
            elif len(pieces) == 1:
                start()
            else:
                pl.when(jnp.logical_and(block >= low, block < high))(start)
            low = high


def fetch_wait(groups, spm, buf_ref, sem_ref):
    for k, pieces in enumerate(groups):
        pltpu.make_async_copy(pieces[0].at[pl.ds(0, spm)], buf_ref.at[k], sem_ref.at[k]).wait()


def cut(refs, counts):
    groups, at = [], 0
    for count in counts:
        groups.append(refs[at : at + count])
        at += count
    return groups, refs[at:]


def owner_block(place_ref, dest, spm):
    return jnp.bitwise_xor(jnp.bitwise_xor(place_ref[0], dest), place_ref[1] // spm)


def attend_block(block, gathered, me, refs, hc, spm):
    weight_ref, bias_ref, gain_ref, shift_ref, labrow, labcol, norm_ref = refs
    n_mp = len(gathered)
    _, width = gathered[0].shape
    full = width * n_mp
    mean = sum(jnp.sum(b, axis=1, keepdims=True) for b in gathered) * (1.0 / full)
    gathered = [b - mean for b in gathered]
    spread = sum(jnp.sum(b * b, axis=1, keepdims=True) for b in gathered) * (1.0 / full)
    scale = lax.rsqrt(spread + 1e-06)
    for k in range(n_mp):
        which = jnp.bitwise_xor(me, k)
        norm_ref[which] = (gathered[k] * scale * gain_ref[which] + shift_ref[which]).astype(BF)
    normed = jnp.concatenate([norm_ref[j] for j in range(n_mp)], axis=1)
    start = hc // LANES * LANES
    lead = hc - start
    qkv = jnp.dot(normed, weight_ref[:, start:], preferred_element_type=F32)
    query = qkv[:, lead : lead + hc] + bias_ref[:, :hc]
    query = (query * (1.0 / math.sqrt(HEAD))).astype(BF)
    key = (qkv[:, lead + hc : lead + 2 * hc] + bias_ref[:, hc : 2 * hc]).astype(BF)
    value = (qkv[:, lead + 2 * hc :] + bias_ref[:, 2 * hc :]).astype(BF)
    slot_rows = labcol.shape[1]
    heads = hc // HEAD
    lane_head = lax.broadcasted_iota(jnp.int32, (slot_rows, hc), 1) // HEAD
    results = []
    for s in range(spm):
        at = slice(s * slot_rows, (s + 1) * slot_rows)
        q, kk, v = query[at], key[at], value[at]
        zero = jnp.zeros_like(q)
        stacked = jnp.concatenate([jnp.where(lane_head == h, q, zero) for h in range(heads)], axis=0)
        scores = lax.dot_general(stacked, kk, NT, preferred_element_type=F32)
        same = labcol[block * spm + s] == labrow[block * spm + s]
        outs = jnp.zeros((slot_rows, hc), F32)
        for h in range(heads):
            sh = jnp.where(same, scores[h * slot_rows : (h + 1) * slot_rows], -jnp.inf)
            e = jnp.exp(sh - jnp.max(sh, axis=1, keepdims=True))
            prob = (e * (1.0 / jnp.sum(e, axis=1, keepdims=True))).astype(BF)
            outs = jnp.where(lane_head == h, jnp.dot(prob, v, preferred_element_type=F32), outs)
        results.append(outs)
    piece = slot_rows // 2
    return [jnp.concatenate([r[:piece], r[piece:]], axis=1).astype(BF) for r in results]


def attend_kernel(counts, blocks, priors, spm, fold, hc, place_ref, *refs):
    n_mp = len(counts)
    groups, refs = cut(refs, counts)
    operands, refs = list(refs[:6]), refs[6:]
    prior_refs, refs = refs[: len(priors)], refs[len(priors) :]
    outs = n_mp * spm if priors else 1
    out_refs, (norm_ref, buf_ref, sem_ref, mine_ref) = refs[:outs], refs[outs:]
    for i, block in enumerate(blocks):
        fetch_start(groups, block, spm, buf_ref.at[i], sem_ref.at[i])

    def one(i, _):
        fetch_wait(groups, spm, buf_ref.at[i], sem_ref.at[i])
        gathered = [unfold(buf_ref[i, k], fold) for k in range(n_mp)]
        values = attend_block(
            blocks[0] + i, gathered, place_ref[0], operands + [norm_ref], hc, spm
        )
        for s, value in enumerate(values):
            (mine_ref if priors else out_refs[0])[i, s] = value
        return 0

    lax.fori_loop(0, len(blocks), one, 0)
    if priors:
        for k in range(n_mp):
            block = owner_block(place_ref, k, spm)
            for s in range(spm):
                value = mine_ref[jnp.maximum(block - blocks[0], 0), s]
                low = 0
                for ref, count in zip(prior_refs, priors):
                    before = ref[jnp.clip(block - low, 0, count - 1), s]
                    value = jnp.where(
                        jnp.logical_and(block >= low, block < low + count), before, value
                    )
                    low += count
                out_refs[k * spm + s][...] = value


def attend(place, gathered, blocks, priors, fold, hc, operands, spm):
    n_mp = len(gathered)
    _, piece, lanes = gathered[0][0].shape
    slot_rows = operands[4].shape[2]
    flat = sum(gathered, [])
    smem = pl.BlockSpec(memory_space=pltpu.SMEM)
    vmem = pl.BlockSpec(memory_space=pltpu.VMEM)
    shape = (slot_rows // 2, 2 * hc)
    if priors:
        out_shape = [jax.ShapeDtypeStruct(shape, BF)] * (n_mp * spm)
    else:
        out_shape = [jax.ShapeDtypeStruct((len(blocks), spm, *shape), BF)]
    outs = pl.pallas_call(
        functools.partial(
            attend_kernel,
            [len(g) for g in gathered],
            blocks,
            [p.shape[0] for p in priors],
            spm,
            fold,
            hc,
        ),
        in_specs=[smem]
        + [pl.BlockSpec(memory_space=pltpu.HBM)] * len(flat)
        + [vmem] * (len(operands) + len(priors)),
        out_specs=[vmem] * len(out_shape),
        scratch_shapes=[
            pltpu.VMEM((n_mp, spm * slot_rows, lanes // fold), BF),
            pltpu.VMEM((len(blocks), n_mp, spm, piece, lanes), BF),
            pltpu.SemaphoreType.DMA((len(blocks), n_mp)),
            pltpu.VMEM((len(blocks), spm, *shape), BF),
        ],
        out_shape=out_shape,
        compiler_params=params(24),
        cost_estimate=cost(len(blocks) * 4e9, operands[0].size * 4),
        name="attend",
    )(place, *flat, *operands, *priors)
    if not priors:
        return outs[0]
    return [outs[k * spm : (k + 1) * spm] for k in range(n_mp)]


def own_kernel(counts, spm, fold, place_ref, *refs):
    n_mp = len(counts)
    groups, (bias_ref, *out_refs, buf_ref, sem_ref) = cut(refs, counts)
    fetch_start(groups, owner_block(place_ref, 0, spm), spm, buf_ref, sem_ref)
    fetch_wait(groups, spm, buf_ref, sem_ref)
    blocks = [unfold(buf_ref[k], fold) for k in range(n_mp)]
    ordered = []
    for j in range(n_mp):
        value = blocks[0]
        for k in range(1, n_mp):
            value = jnp.where(jnp.bitwise_xor(place_ref[0], k) == j, blocks[k], value)
        ordered.append(value)
    value = jnp.concatenate(ordered, axis=1) + bias_ref[...]
    rows = value.shape[0] // spm
    for s in range(spm):
        out_refs[s][...] = value[s * rows : (s + 1) * rows]


def own_rows(place, gathered, fold, bias, spm):
    n_mp = len(gathered)
    _, piece, lanes = gathered[0][0].shape
    features = sum(gathered, [])
    vmem = pl.BlockSpec(memory_space=pltpu.VMEM)
    return pl.pallas_call(
        functools.partial(own_kernel, [len(g) for g in gathered], spm, fold),
        in_specs=[pl.BlockSpec(memory_space=pltpu.SMEM)]
        + [pl.BlockSpec(memory_space=pltpu.HBM)] * len(features)
        + [vmem],
        out_specs=[vmem] * spm,
        out_shape=[jax.ShapeDtypeStruct((piece * fold, bias.shape[1]), F32)] * spm,
        scratch_shapes=[
            pltpu.VMEM((n_mp, spm, piece, lanes), BF),
            pltpu.SemaphoreType.DMA((n_mp,)),
        ],
        compiler_params=params(16),
        cost_estimate=cost(1e9, 4 * bias.size * piece),
        name="own",
    )(place, *features, bias)


def project_kernel(out_counts, hc, place_ref, base_ref, *refs):
    n_mp = len(out_counts)
    att_refs, at = refs[:n_mp], n_mp
    own_ref, at = refs[at], at + 1
    half = own_ref.shape[0] // 2
    core = place_ref[1] % 2
    mine, mate = None, None
    for k, count in enumerate(out_counts):
        left = jnp.concatenate([att_refs[k][:, :hc], att_refs[k][:, hc:]], axis=0)
        if k == 0:
            pair = [
                [own_ref[pl.ds(pl.multiple_of(c * half, 128), half)]] for c in (core, 1 - core)
            ]
        else:
            pair = [[r[...] for r in refs[at : at + count]], [r[...] for r in refs[at + count : at + 2 * count]]]
            at += 2 * count
        sums = [
            jnp.concatenate(
                [lax.dot_general(left, w, NT, preferred_element_type=F32) for w in ws], axis=1
            )
            for ws in pair
        ]
        mine, mate = (sums[0], sums[1]) if mine is None else (mine + sums[0], mate + sums[1])
    total = jnp.concatenate(
        [jnp.where(core == 0, mine, mate), jnp.where(core == 0, mate, mine)], axis=1
    )
    gain_ref, shift_ref, _, res_ref, out_ref = refs[at:]
    value = base_ref[...] + total
    res_ref[...] = value
    mean = jnp.mean(value, axis=1, keepdims=True)
    value = value - mean
    spread = jnp.mean(value * value, axis=1, keepdims=True)
    out_ref[...] = (value * lax.rsqrt(spread + 1e-06) * gain_ref[...] + shift_ref[...]).astype(BF)


def project(place, base, hc, attended, out_weights, gain, shift, last):
    n_mp = len(attended)
    weights = sum([sum(w, []) for w in out_weights], [])
    vmem = pl.BlockSpec(memory_space=pltpu.VMEM)
    return pl.pallas_call(
        functools.partial(project_kernel, [len(w[0]) for w in out_weights], hc),
        in_specs=[pl.BlockSpec(memory_space=pltpu.SMEM)]
        + [vmem] * (n_mp + len(weights) + 3)
        + [pl.BlockSpec(memory_space=pl.ANY)],
        out_specs=[vmem] * 2,
        out_shape=[jax.ShapeDtypeStruct(base.shape, F32), jax.ShapeDtypeStruct(base.shape, BF)],
        compiler_params=params(20),
        cost_estimate=cost(2e9, 16 * base.size),
        name="project",
    )(place, base, *attended, *weights, gain, shift, last)


def mlp_kernel(count, *refs):
    in_refs, (weight_ref, bias_ref), out_refs = refs[:count], refs[count : count + 2], refs[count + 3 :]
    rows = jnp.concatenate([r[...] for r in in_refs], axis=0)
    hidden_width = bias_ref.shape[1]
    step = 256 if hidden_width % 256 == 0 else LANES
    hidden = []
    for c in range(0, hidden_width, step):
        at = slice(c, c + step)
        up = jnp.dot(rows, weight_ref[:, at], preferred_element_type=F32) + bias_ref[:, at]
        hidden.append((0.5 * up * (1.0 + lax.erf(up * math.sqrt(0.5)))).astype(BF))
    hidden = jnp.concatenate(hidden, axis=1)
    each, width = out_refs[0].shape
    for c in range(0, width, 256):
        part = lax.dot_general(
            hidden, weight_ref[c : c + 256, hidden_width:], NT, preferred_element_type=F32
        )
        for i, ref in enumerate(out_refs):
            ref[:, c : c + 256] = part[i * each : (i + 1) * each].astype(BF)


def mlp(rows, outs, weight, bias, after):
    width = weight.shape[0]
    total = sum(r.shape[0] for r in rows)
    vmem = pl.BlockSpec(memory_space=pltpu.VMEM)
    return pl.pallas_call(
        functools.partial(mlp_kernel, len(rows)),
        in_specs=[vmem] * (len(rows) + 2) + [pl.BlockSpec(memory_space=pl.ANY)],
        out_specs=[vmem] * outs,
        out_shape=[jax.ShapeDtypeStruct((total // outs, width), BF)] * outs,
        compiler_params=params(20),
        cost_estimate=cost(total * weight.size * 2, weight.size * 2),
    )(*rows, weight, bias, after)


def settle_kernel(adds, pieces, *refs):
    add_refs, res_refs, bias_ref, out_refs = (
        refs[:adds],
        refs[adds : adds + pieces],
        refs[adds + pieces],
        refs[adds + pieces + 1 :],
    )
    for s in range(pieces):
        value = res_refs[s][...] + bias_ref[...]
        for i in range(s, adds, pieces):
            value = value + add_refs[i][...].astype(F32)
        out_refs[s][...] = value


def settle(added, residual, bias):
    vmem = pl.BlockSpec(memory_space=pltpu.VMEM)
    return pl.pallas_call(
        functools.partial(settle_kernel, len(added), len(residual)),
        in_specs=[vmem] * (len(added) + len(residual) + 1),
        out_specs=[vmem] * len(residual),
        out_shape=[jax.ShapeDtypeStruct(r.shape, F32) for r in residual],
        compiler_params=params(16),
        cost_estimate=cost(1e9, residual[0].size * 24),
        name="settle",
    )(*added, *residual, bias)


def finish_kernel(adds, pieces, place_ref, *refs):
    add_refs, res_refs, lab_ref, out_ref = (
        refs[:adds],
        refs[adds : adds + pieces],
        refs[adds + pieces],
        refs[adds + pieces + 1],
    )
    each = res_refs[0].shape[0]
    turn = place_ref[1] % pieces
    for s in range(pieces):
        value = res_refs[s][...]
        for i in range(s, adds, pieces):
            value = value + add_refs[i][...].astype(F32)
        value = jnp.where(lab_ref[s] >= 0, value, 0.0).astype(BF)
        out_ref[pl.ds(pl.multiple_of(jnp.bitwise_xor(turn, s) * each, 16), each)] = value


def finish(place, added, residual, labels):
    smem = pl.BlockSpec(memory_space=pltpu.SMEM)
    vmem = pl.BlockSpec(memory_space=pltpu.VMEM)
    rows, width = residual[0].shape
    return pl.pallas_call(
        functools.partial(finish_kernel, len(added), len(residual)),
        in_specs=[smem] + [vmem] * (len(added) + len(residual) + 1),
        out_specs=vmem,
        out_shape=jax.ShapeDtypeStruct((rows * len(residual), width), BF),
        compiler_params=params(16),
        cost_estimate=cost(1e9, rows * width * 16),
        name="finish",
    )(place, *added, *residual, labels)


def hop(value, k, n):
    return lax.ppermute(value, "mp", [(i, i ^ k) for i in range(n)])


def gather_blocks(values, n, direct=False):
    if n != 4:
        return [values] + [[hop(v, k, n) for v in values] for k in range(1, n)]
    x, y = [], []
    for v in values:
        x.append(hop(v, 1, n))
        y.append(hop(v, 2, n))
    if direct:
        return [values, x, y, [hop(v, 3, n) for v in values]]
    half = values[0].shape[0] // 2
    top, bottom = (x[0], y[1]) if len(values) == 2 else (x[0][:half], y[0][half:])
    far = [hop(top, 2, n), hop(bottom, 1, n)]
    return [values, x, y, far]


def plus(a, b):
    return (a.astype(F32) + b.astype(F32)).astype(BF)


def scatter_blocks(partials, n):
    own = list(partials[0])
    if n != 4 or len(own) != 2:
        return own, [hop(p, k, n) for k in range(1, n) for p in partials[k]]
    far, x, y = partials[3], partials[1], partials[2]
    x0, y1 = hop(x[0], 1, n), hop(y[1], 2, n)
    first, second = hop(far[0], 1, n), hop(far[1], 2, n)
    y0, x1 = hop(plus(y[0], first), 2, n), hop(plus(x[1], second), 1, n)
    return own + [x0, y1], [y0, x1]


def per_device(
    patches,
    position,
    keep,
    counts,
    offsets,
    ln_gain,
    ln_bias,
    w_qkv,
    b_qkv,
    w_o,
    b_o,
    w_up,
    b_up,
    w_down,
    b_down,
):
    local_images, _, width = patches.shape
    keep_most = keep.shape[1]
    n_dp, n_mp = lax.axis_size("dp"), lax.axis_size("mp")
    d, m = lax.axis_index("dp"), lax.axis_index("mp")
    images_here = local_images * n_mp
    per_slot = (images_here + n_dp - 1) // n_dp
    slot_rows = max(keep_most + 16, per_slot * keep_most * 5 // 8)
    pack_rows = slot_rows * n_dp
    spm = n_dp // n_mp
    feat = width // n_mp
    hc = w_qkv.shape[3]
    place = jnp.stack([m, d]).astype(jnp.int32)

    mixed = join(w_qkv[0], w_o[0].T)
    mixed = lax.all_gather(mixed, "dp", axis=0, tiled=True)
    tokens = embed(place, patches, position, keep, n_mp)
    featured = [tokens[0]] + [hop(tokens[k], k, n_mp) for k in range(1, n_mp)]

    own = mixed[:, :hc]
    part = lax.dynamic_slice_in_dim(own, (d % 2) * (width // 2), width // 2)
    mate = [(i, i ^ 1) for i in range(n_dp)]
    out_weights = [[[own]]]
    for pieces in gather_blocks([part], n_mp)[1:]:
        out_weights.append([pieces, [lax.ppermute(p, "dp", mate) for p in pieces]])

    first_image = d * images_here
    group_counts = lax.dynamic_slice_in_dim(counts, first_image, images_here)
    group_offsets = lax.dynamic_slice_in_dim(offsets, first_image, images_here)
    shard_index = group_offsets // pack_rows
    base_row = shard_index * slot_rows + group_offsets - shard_index * pack_rows - d * slot_rows
    spot = jnp.arange(keep_most, dtype=jnp.int32)
    target = jnp.where(
        spot[None, :] < group_counts[:, None], base_row[:, None] + spot[None, :], pack_rows
    ).reshape(n_mp, 1, local_images * keep_most)
    fold = 2
    packed = pack(place, featured, target, n_dp, slot_rows, fold)
    half = n_dp // 2
    bounds = [0, half, n_dp]
    moved = [packed[0]]
    for i in range(1, n_dp):
        moved.append(lax.ppermute(packed[i], "dp", [(j, j ^ i) for j in range(n_dp)]))
    stacks = []
    for i in range(2):
        stacks.append(jnp.stack(moved[bounds[i] : bounds[i + 1]]))
    both = jnp.concatenate([w_up[0], w_down[0].T], axis=1)
    both = lax.all_gather(both, "dp", axis=0, tiled=True)

    image_ids = jnp.arange(counts.shape[0], dtype=jnp.int32)
    slots = jnp.bitwise_xor(jnp.arange(n_dp, dtype=jnp.int32), d)
    packed_rows = d * pack_rows + slots[:, None] * slot_rows + jnp.arange(slot_rows, dtype=jnp.int32)
    packed_rows = packed_rows.reshape(pack_rows)
    inside = (packed_rows[:, None] >= offsets[None, :]) & (
        packed_rows[:, None] < (offsets + counts)[None, :]
    )
    labels = jnp.max(jnp.where(inside, image_ids[None, :] + 1, 0), axis=1) - 1
    labrow = labels.reshape(n_dp, 1, slot_rows)
    labcol = labels.reshape(n_dp, slot_rows, 1)

    moved = [gather_blocks([v], n_mp, i > 0) for i, v in enumerate(stacks)]
    gain = ln_gain[0, 0].reshape(n_mp, 1, feat)
    shift = ln_bias[0, 0].reshape(n_mp, 1, feat)
    bias = b_qkv[0].reshape(1, 3 * hc)
    operands = (mixed, bias, gain, shift, labrow, labcol)
    priors = []
    for i in range(2):
        gathered = [sum(pieces, []) for pieces in zip(*moved[: i + 1])]
        attended = attend(
            place,
            gathered,
            list(range(bounds[i] // spm, bounds[i + 1] // spm)),
            priors if i else [],
            fold,
            hc,
            operands,
            spm,
        )
        priors.append(attended)
    pieces = []
    for s in range(spm):
        pieces.append(
            [attended[0][s]] + [hop(attended[k][s], k, n_mp) for k in range(1, n_mp)]
        )
    base = own_rows(place, gathered, fold, b_o, spm)
    residual, normed = [], []
    last = base[0]
    for s in range(spm):
        kept, last = project(
            place, base[s], hc, pieces[s], out_weights, ln_gain[0, 1:2], ln_bias[0, 1:2], last
        )
        residual.append(kept)
        normed.append(last)
    blocks = gather_blocks(normed, n_mp)
    partials = [[None] * spm for _ in range(n_mp)]
    last = normed[0]
    if n_mp == 4 and spm == 2:
        groups = [[(0, 0), (0, 1)], [(1, 0), (2, 1)], [(1, 1), (2, 0)], [(3, 0), (3, 1)]]
    else:
        groups = [[(k, i) for i in range(spm)] for k in range(n_mp)]
    for group in groups:
        outs = mlp([blocks[k][i] for k, i in group], len(group), both, b_up, last)
        last = outs[0]
        for (k, i), out in zip(group, outs):
            partials[k][i] = out
    early, late = scatter_blocks(partials, n_mp)
    settled = settle(early, residual, b_down)
    own_labels = lax.dynamic_slice_in_dim(labcol, jnp.bitwise_xor(m, d // spm) * spm, spm)
    return finish(place, late, settled, own_labels)


def solution(mesh):
    in_specs = (
        P(("dp", "mp"), None, None),
        P(),
        P(("dp", "mp"), None),
        P(),
        P(),
        P(),
        P(),
        P(None, None, "dp", "mp"),
        P(None, None, "mp"),
        P(None, "mp", "dp"),
        P(),
        P(None, "dp", "mp"),
        P(None, "mp"),
        P(None, "mp", "dp"),
        P(),
    )
    out_specs = P(("dp", "mp"), None)

    return jax.shard_map(
        per_device, mesh=mesh, in_specs=in_specs, out_specs=out_specs, check_vma=False
    )
```

```python
import functools
import math

import jax
import jax.numpy as jnp
from jax import lax
from jax.experimental import pallas as pl
from jax.experimental.pallas import tpu as pltpu
from jax.sharding import PartitionSpec as P


HEAD = 80
LANES = 128
BF = jnp.bfloat16
F32 = jnp.float32
NT = (((1,), (1,)), ((), ()))


def cost(flops, moved):
    return pl.CostEstimate(flops=int(flops), bytes_accessed=int(moved), transcendentals=0)


def params(mib=48):
    return pltpu.CompilerParams(vmem_limit_bytes=mib * 1024 * 1024)


def embed_kernel(place_ref, keep_ref, patches_ref, position_ref, *refs):
    out_refs, token_ref = refs[:-1], refs[-1]
    per, patch_count, _ = patches_ref.shape
    first = pl.program_id(0) * per
    row = jnp.concatenate([keep_ref[pl.ds(first + i, 1)] for i in range(per)], axis=1).astype(F32)
    tokens = row.shape[1]
    kept = jnp.broadcast_to(row, (tokens, tokens)).T
    reps = (patch_count + tokens - 1) // tokens
    wide = jnp.concatenate([kept] * reps, axis=1)[:, :patch_count]
    lane = lax.broadcasted_iota(jnp.int32, (tokens, patch_count), 1).astype(F32)
    onehot = jnp.where(wide == lane, 1.0, 0.0).astype(BF)
    each = tokens // per
    placed = jnp.dot(onehot, position_ref[...], preferred_element_type=F32)
    picked = jnp.concatenate(
        [
            jnp.dot(onehot[i * each : (i + 1) * each], patches_ref[i], preferred_element_type=F32)
            for i in range(per)
        ],
        axis=0,
    )
    token_ref[...] = (picked + placed).T.astype(BF).reshape(token_ref.shape)
    for k, ref in enumerate(out_refs):
        ref[...] = token_ref[jnp.bitwise_xor(place_ref[0], k)]


def embed(place, patches, position, keep, n_mp):
    images, patch_count, width = patches.shape
    keep_most = keep.shape[1]
    per = max(1, min(images, LANES // keep_most))
    steps = images // per
    tokens = per * keep_most
    return pl.pallas_call(
        embed_kernel,
        grid=(steps,),
        in_specs=[
            pl.BlockSpec(memory_space=pltpu.SMEM),
            pl.BlockSpec(keep.shape, lambda i: (0, 0)),
            pl.BlockSpec((per, patch_count, width), lambda i: (i, 0, 0)),
            pl.BlockSpec((patch_count, width), lambda i: (0, 0)),
        ],
        out_specs=[pl.BlockSpec((width // n_mp, tokens), lambda i: (0, i))] * n_mp,
        out_shape=[jax.ShapeDtypeStruct((width // n_mp, images * keep_most), BF)] * n_mp,
        scratch_shapes=[pltpu.VMEM((n_mp, width // n_mp, tokens), BF)],
        compiler_params=params(60),
        cost_estimate=cost(4e9, patches.size * 2),
        name="embed",
    )(place, keep, patches, position)


def join_kernel(qkv_ref, out_ref, joined_ref):
    joined_ref[...] = jnp.concatenate(
        [out_ref[...]] + [qkv_ref[t] for t in range(qkv_ref.shape[0])], axis=1
    )


def join(w_qkv, w_o):
    kinds, rows, width = w_qkv.shape
    vmem = pl.BlockSpec(memory_space=pltpu.VMEM)
    return pl.pallas_call(
        join_kernel,
        in_specs=[vmem] * 2,
        out_specs=vmem,
        out_shape=jax.ShapeDtypeStruct((rows, (kinds + 1) * width), BF),
        compiler_params=params(60),
        cost_estimate=cost(1e8, 4 * rows * kinds * width),
        name="join",
    )(w_qkv, w_o)


def pack_kernel(fold, slot_rows, group, n_src, place_ref, target_ref, *refs):
    feat_refs, out_refs = refs[:n_src], refs[n_src:]
    width, tokens = feat_refs[0].shape
    d = place_ref[1]
    piece = slot_rows // fold
    for g in range(0, len(out_refs), group):
        row = jnp.concatenate(
            [
                lax.broadcasted_iota(jnp.int32, (slot_rows, tokens), 0)
                + jnp.bitwise_xor(d, g + b) * slot_rows
                for b in range(group)
            ],
            axis=0,
        )
        total = jnp.zeros((group * slot_rows, width), F32)
        for j in range(n_src):
            at = jnp.bitwise_xor(place_ref[0], j)
            onehot = jnp.where(row == target_ref[at], 1.0, 0.0).astype(BF)
            total = total + lax.dot_general(onehot, feat_refs[j][...], NT, preferred_element_type=F32)
        for b in range(group):
            start = b * slot_rows
            chunks = [total[start + f * piece : start + (f + 1) * piece] for f in range(fold)]
            out_refs[g + b][...] = jnp.concatenate(chunks, axis=1).astype(BF)


def pack(place, featured, target, slots, slot_rows, fold):
    width, tokens = featured[0].shape
    smem = pl.BlockSpec(memory_space=pltpu.SMEM)
    vmem = pl.BlockSpec(memory_space=pltpu.VMEM)
    return pl.pallas_call(
        functools.partial(pack_kernel, fold, slot_rows, min(4, slots), len(featured)),
        in_specs=[smem] + [vmem] * (1 + len(featured)),
        out_specs=[vmem] * slots,
        out_shape=[jax.ShapeDtypeStruct((slot_rows // fold, fold * width), BF)] * slots,
        compiler_params=params(24),
        cost_estimate=cost(4e9, width * tokens * 8),
        name="pack",
    )(place, target, *featured)


def unfold(values, fold):
    width = values.shape[2] // fold
    values = values.astype(F32)
    pieces = [
        values[s, :, f * width : (f + 1) * width] for s in range(values.shape[0]) for f in range(fold)
    ]
    return jnp.concatenate(pieces, axis=0)


def fetch_start(groups, block, spm, buf_ref, sem_ref):
    for k, pieces in enumerate(groups):
        low = 0
        for piece in pieces:
            high = low + piece.shape[0] // spm

            def start(piece=piece, k=k, low=low):
                at = pl.ds((block - low) * spm, spm)
                pltpu.make_async_copy(piece.at[at], buf_ref.at[k], sem_ref.at[k]).start()

            if isinstance(block, int):
                if low <= block < high:
                    start()
            elif len(pieces) == 1:
                start()
            else:
                pl.when(jnp.logical_and(block >= low, block < high))(start)
            low = high


def fetch_wait(groups, spm, buf_ref, sem_ref):
    for k, pieces in enumerate(groups):
        pltpu.make_async_copy(pieces[0].at[pl.ds(0, spm)], buf_ref.at[k], sem_ref.at[k]).wait()


def cut(refs, counts):
    groups, at = [], 0
    for count in counts:
        groups.append(refs[at : at + count])
        at += count
    return groups, refs[at:]


def owner_block(place_ref, dest, spm):
    return jnp.bitwise_xor(jnp.bitwise_xor(place_ref[0], dest), place_ref[1] // spm)


def attend_block(block, gathered, me, refs, hc, spm):
    weight_ref, bias_ref, gain_ref, shift_ref, labrow, labcol, norm_ref = refs
    n_mp = len(gathered)
    _, width = gathered[0].shape
    full = width * n_mp
    mean = sum(jnp.sum(b, axis=1, keepdims=True) for b in gathered) * (1.0 / full)
    gathered = [b - mean for b in gathered]
    spread = sum(jnp.sum(b * b, axis=1, keepdims=True) for b in gathered) * (1.0 / full)
    scale = lax.rsqrt(spread + 1e-06)
    for k in range(n_mp):
        which = jnp.bitwise_xor(me, k)
        norm_ref[which] = (gathered[k] * scale * gain_ref[which] + shift_ref[which]).astype(BF)
    normed = jnp.concatenate([norm_ref[j] for j in range(n_mp)], axis=1)
    start = hc // LANES * LANES
    lead = hc - start
    qkv = jnp.dot(normed, weight_ref[:, start:], preferred_element_type=F32)
    query = qkv[:, lead : lead + hc] + bias_ref[:, :hc]
    query = (query * (1.0 / math.sqrt(HEAD))).astype(BF)
    key = (qkv[:, lead + hc : lead + 2 * hc] + bias_ref[:, hc : 2 * hc]).astype(BF)
    value = (qkv[:, lead + 2 * hc :] + bias_ref[:, 2 * hc :]).astype(BF)
    slot_rows = labcol.shape[1]
    heads = hc // HEAD
    lane_head = lax.broadcasted_iota(jnp.int32, (slot_rows, hc), 1) // HEAD
    results = []
    for s in range(spm):
        at = slice(s * slot_rows, (s + 1) * slot_rows)
        q, kk, v = query[at], key[at], value[at]
        zero = jnp.zeros_like(q)
        stacked = jnp.concatenate([jnp.where(lane_head == h, q, zero) for h in range(heads)], axis=0)
        scores = lax.dot_general(stacked, kk, NT, preferred_element_type=F32)
        same = labcol[block * spm + s] == labrow[block * spm + s]
        outs = jnp.zeros((slot_rows, hc), F32)
        for h in range(heads):
            sh = jnp.where(same, scores[h * slot_rows : (h + 1) * slot_rows], -jnp.inf)
            e = jnp.exp(sh - jnp.max(sh, axis=1, keepdims=True))
            prob = (e * (1.0 / jnp.sum(e, axis=1, keepdims=True))).astype(BF)
            outs = jnp.where(lane_head == h, jnp.dot(prob, v, preferred_element_type=F32), outs)
        results.append(outs)
    piece = slot_rows // 2
    return [jnp.concatenate([r[:piece], r[piece:]], axis=1).astype(BF) for r in results]


def attend_kernel(counts, blocks, priors, spm, fold, hc, place_ref, *refs):
    n_mp = len(counts)
    groups, refs = cut(refs, counts)
    operands, refs = list(refs[:6]), refs[6:]
    prior_refs, refs = refs[: len(priors)], refs[len(priors) :]
    outs = n_mp * spm if priors else 1
    out_refs, (norm_ref, buf_ref, sem_ref, mine_ref) = refs[:outs], refs[outs:]
    for i, block in enumerate(blocks):
        fetch_start(groups, block, spm, buf_ref.at[i], sem_ref.at[i])

    def one(i, _):
        fetch_wait(groups, spm, buf_ref.at[i], sem_ref.at[i])
        gathered = [unfold(buf_ref[i, k], fold) for k in range(n_mp)]
        values = attend_block(
            blocks[0] + i, gathered, place_ref[0], operands + [norm_ref], hc, spm
        )
        for s, value in enumerate(values):
            (mine_ref if priors else out_refs[0])[i, s] = value
        return 0

    lax.fori_loop(0, len(blocks), one, 0)
    if priors:
        for k in range(n_mp):
            block = owner_block(place_ref, k, spm)
            for s in range(spm):
                value = mine_ref[jnp.maximum(block - blocks[0], 0), s]
                low = 0
                for ref, count in zip(prior_refs, priors):
                    before = ref[jnp.clip(block - low, 0, count - 1), s]
                    value = jnp.where(
                        jnp.logical_and(block >= low, block < low + count), before, value
                    )
                    low += count
                out_refs[k * spm + s][...] = value


def attend(place, gathered, blocks, priors, fold, hc, operands, spm):
    n_mp = len(gathered)
    _, piece, lanes = gathered[0][0].shape
    slot_rows = operands[4].shape[2]
    flat = sum(gathered, [])
    smem = pl.BlockSpec(memory_space=pltpu.SMEM)
    vmem = pl.BlockSpec(memory_space=pltpu.VMEM)
    shape = (slot_rows // 2, 2 * hc)
    if priors:
        out_shape = [jax.ShapeDtypeStruct(shape, BF)] * (n_mp * spm)
    else:
        out_shape = [jax.ShapeDtypeStruct((len(blocks), spm, *shape), BF)]
    outs = pl.pallas_call(
        functools.partial(
            attend_kernel,
            [len(g) for g in gathered],
            blocks,
            [p.shape[0] for p in priors],
            spm,
            fold,
            hc,
        ),
        in_specs=[smem]
        + [pl.BlockSpec(memory_space=pltpu.HBM)] * len(flat)
        + [vmem] * (len(operands) + len(priors)),
        out_specs=[vmem] * len(out_shape),
        scratch_shapes=[
            pltpu.VMEM((n_mp, spm * slot_rows, lanes // fold), BF),
            pltpu.VMEM((len(blocks), n_mp, spm, piece, lanes), BF),
            pltpu.SemaphoreType.DMA((len(blocks), n_mp)),
            pltpu.VMEM((len(blocks), spm, *shape), BF),
        ],
        out_shape=out_shape,
        compiler_params=params(14),
        cost_estimate=cost(len(blocks) * 4e9, operands[0].size * 4),
        name="attend",
    )(place, *flat, *operands, *priors)
    if not priors:
        return outs[0]
    return [outs[k * spm : (k + 1) * spm] for k in range(n_mp)]


def own_kernel(counts, spm, fold, place_ref, *refs):
    n_mp = len(counts)
    groups, (bias_ref, *out_refs, buf_ref, sem_ref) = cut(refs, counts)
    fetch_start(groups, owner_block(place_ref, 0, spm), spm, buf_ref, sem_ref)
    fetch_wait(groups, spm, buf_ref, sem_ref)
    blocks = [unfold(buf_ref[k], fold) for k in range(n_mp)]
    ordered = []
    for j in range(n_mp):
        value = blocks[0]
        for k in range(1, n_mp):
            value = jnp.where(jnp.bitwise_xor(place_ref[0], k) == j, blocks[k], value)
        ordered.append(value)
    value = jnp.concatenate(ordered, axis=1) + bias_ref[...]
    rows = value.shape[0] // spm
    for s in range(spm):
        out_refs[s][...] = value[s * rows : (s + 1) * rows]


def own_rows(place, gathered, fold, bias, spm):
    n_mp = len(gathered)
    _, piece, lanes = gathered[0][0].shape
    features = sum(gathered, [])
    vmem = pl.BlockSpec(memory_space=pltpu.VMEM)
    return pl.pallas_call(
        functools.partial(own_kernel, [len(g) for g in gathered], spm, fold),
        in_specs=[pl.BlockSpec(memory_space=pltpu.SMEM)]
        + [pl.BlockSpec(memory_space=pltpu.HBM)] * len(features)
        + [vmem],
        out_specs=[vmem] * spm,
        out_shape=[jax.ShapeDtypeStruct((piece * fold, bias.shape[1]), F32)] * spm,
        scratch_shapes=[
            pltpu.VMEM((n_mp, spm, piece, lanes), BF),
            pltpu.SemaphoreType.DMA((n_mp,)),
        ],
        compiler_params=params(16),
        cost_estimate=cost(1e9, 4 * bias.size * piece),
        name="own",
    )(place, *features, bias)


def project_kernel(out_counts, hc, place_ref, base_ref, *refs):
    n_mp = len(out_counts)
    att_refs, at = refs[:n_mp], n_mp
    own_ref, at = refs[at], at + 1
    half = own_ref.shape[0] // 2
    core = place_ref[1] % 2
    mine, mate = None, None
    for k, count in enumerate(out_counts):
        left = jnp.concatenate([att_refs[k][:, :hc], att_refs[k][:, hc:]], axis=0)
        if k == 0:
            sums = [
                lax.dot_general(
                    left,
                    own_ref[pl.ds(pl.multiple_of(c * half, 128), half)],
                    NT,
                    preferred_element_type=F32,
                )
                for c in (core, 1 - core)
            ]
        else:
            zero = jnp.zeros_like(left)
            both = jnp.concatenate(
                [jnp.concatenate([left, zero], axis=1), jnp.concatenate([zero, left], axis=1)], axis=0
            )
            sums = []
            for _ in range(2):
                part = jnp.concatenate(
                    [
                        lax.dot_general(both, r[...], NT, preferred_element_type=F32)
                        for r in refs[at : at + count]
                    ],
                    axis=1,
                )
                rows = left.shape[0]
                sums.append(jnp.concatenate([part[:rows], part[rows:]], axis=1))
                at += count
        mine, mate = (sums[0], sums[1]) if mine is None else (mine + sums[0], mate + sums[1])
    total = jnp.concatenate(
        [jnp.where(core == 0, mine, mate), jnp.where(core == 0, mate, mine)], axis=1
    )
    gain_ref, shift_ref, _, res_ref, out_ref = refs[at:]
    value = base_ref[...] + total
    res_ref[...] = value
    mean = jnp.mean(value, axis=1, keepdims=True)
    value = value - mean
    spread = jnp.mean(value * value, axis=1, keepdims=True)
    out_ref[...] = (value * lax.rsqrt(spread + 1e-06) * gain_ref[...] + shift_ref[...]).astype(BF)


def project(place, base, hc, attended, out_weights, gain, shift, last):
    n_mp = len(attended)
    weights = sum([sum(w, []) for w in out_weights], [])
    vmem = pl.BlockSpec(memory_space=pltpu.VMEM)
    return pl.pallas_call(
        functools.partial(project_kernel, [len(w[0]) for w in out_weights], hc),
        in_specs=[pl.BlockSpec(memory_space=pltpu.SMEM)]
        + [vmem] * (n_mp + len(weights) + 3)
        + [pl.BlockSpec(memory_space=pl.ANY)],
        out_specs=[vmem] * 2,
        out_shape=[jax.ShapeDtypeStruct(base.shape, F32), jax.ShapeDtypeStruct(base.shape, BF)],
        compiler_params=params(12),
        cost_estimate=cost(2e9, 16 * base.size),
        name="project",
    )(place, base, *attended, *weights, gain, shift, last)


def mlp_kernel(count, *refs):
    in_refs, (weight_ref, bias_ref), out_refs = refs[:count], refs[count : count + 2], refs[count + 3 :]
    rows = jnp.concatenate([r[...] for r in in_refs], axis=0)
    hidden_width = bias_ref.shape[1]
    step = 256 if hidden_width % 256 == 0 else LANES
    hidden = []
    for c in range(0, hidden_width, step):
        at = slice(c, c + step)
        up = jnp.dot(rows, weight_ref[:, at], preferred_element_type=F32) + bias_ref[:, at]
        hidden.append((0.5 * up * (1.0 + lax.erf(up * math.sqrt(0.5)))).astype(BF))
    hidden = jnp.concatenate(hidden, axis=1)
    each, width = out_refs[0].shape
    for c in range(0, width, 256):
        part = lax.dot_general(
            hidden, weight_ref[c : c + 256, hidden_width:], NT, preferred_element_type=F32
        )
        for i, ref in enumerate(out_refs):
            ref[:, c : c + 256] = part[i * each : (i + 1) * each].astype(BF)


def mlp(rows, outs, weight, bias, after):
    width = weight.shape[0]
    total = sum(r.shape[0] for r in rows)
    vmem = pl.BlockSpec(memory_space=pltpu.VMEM)
    return pl.pallas_call(
        functools.partial(mlp_kernel, len(rows)),
        in_specs=[vmem] * (len(rows) + 2) + [pl.BlockSpec(memory_space=pl.ANY)],
        out_specs=[vmem] * outs,
        out_shape=[jax.ShapeDtypeStruct((total // outs, width), BF)] * outs,
        compiler_params=params(20),
        cost_estimate=cost(total * weight.size * 2, weight.size * 2),
    )(*rows, weight, bias, after)


def settle_kernel(adds, pieces, *refs):
    add_refs, res_refs, bias_ref, out_refs = (
        refs[:adds],
        refs[adds : adds + pieces],
        refs[adds + pieces],
        refs[adds + pieces + 1 :],
    )
    for s in range(pieces):
        value = res_refs[s][...] + bias_ref[...]
        for i in range(s, adds, pieces):
            value = value + add_refs[i][...].astype(F32)
        out_refs[s][...] = value


def settle(added, residual, bias):
    vmem = pl.BlockSpec(memory_space=pltpu.VMEM)
    return pl.pallas_call(
        functools.partial(settle_kernel, len(added), len(residual)),
        in_specs=[vmem] * (len(added) + len(residual) + 1),
        out_specs=[vmem] * len(residual),
        out_shape=[jax.ShapeDtypeStruct(r.shape, F32) for r in residual],
        compiler_params=params(16),
        cost_estimate=cost(1e9, residual[0].size * 24),
        name="settle",
    )(*added, *residual, bias)


def finish_kernel(adds, pieces, place_ref, *refs):
    add_refs, res_refs, lab_ref, out_ref = (
        refs[:adds],
        refs[adds : adds + pieces],
        refs[adds + pieces],
        refs[adds + pieces + 1],
    )
    each = res_refs[0].shape[0]
    turn = place_ref[1] % pieces
    for s in range(pieces):
        value = res_refs[s][...]
        for i in range(s, adds, pieces):
            value = value + add_refs[i][...].astype(F32)
        value = jnp.where(lab_ref[s] >= 0, value, 0.0).astype(BF)
        out_ref[pl.ds(pl.multiple_of(jnp.bitwise_xor(turn, s) * each, 16), each)] = value


def finish(place, added, residual, labels):
    smem = pl.BlockSpec(memory_space=pltpu.SMEM)
    vmem = pl.BlockSpec(memory_space=pltpu.VMEM)
    rows, width = residual[0].shape
    return pl.pallas_call(
        functools.partial(finish_kernel, len(added), len(residual)),
        in_specs=[smem] + [vmem] * (len(added) + len(residual) + 1),
        out_specs=vmem,
        out_shape=jax.ShapeDtypeStruct((rows * len(residual), width), BF),
        compiler_params=params(16),
        cost_estimate=cost(1e9, rows * width * 16),
        name="finish",
    )(place, *added, *residual, labels)


def hop(value, k, n):
    return lax.ppermute(value, "mp", [(i, i ^ k) for i in range(n)])


def gather_blocks(values, n, direct=False):
    if n != 4:
        return [values] + [[hop(v, k, n) for v in values] for k in range(1, n)]
    x, y = [], []
    for v in values:
        x.append(hop(v, 1, n))
        y.append(hop(v, 2, n))
    if direct:
        return [values, x, y, [hop(v, 3, n) for v in values]]
    half = values[0].shape[0] // 2
    top, bottom = (x[0], y[1]) if len(values) == 2 else (x[0][:half], y[0][half:])
    far = [hop(top, 2, n), hop(bottom, 1, n)]
    return [values, x, y, far]


def plus(a, b):
    return (a.astype(F32) + b.astype(F32)).astype(BF)


def scatter_blocks(partials, n):
    own = list(partials[0])
    if n != 4 or len(own) != 2:
        return own, [hop(p, k, n) for k in range(1, n) for p in partials[k]]
    far, x, y = partials[3], partials[1], partials[2]
    x0, y1 = hop(x[0], 1, n), hop(y[1], 2, n)
    first, second = hop(far[0], 1, n), hop(far[1], 2, n)
    y0, x1 = hop(plus(y[0], first), 2, n), hop(plus(x[1], second), 1, n)
    return own + [x0, y1], [y0, x1]


def per_device(
    patches,
    position,
    keep,
    counts,
    offsets,
    ln_gain,
    ln_bias,
    w_qkv,
    b_qkv,
    w_o,
    b_o,
    w_up,
    b_up,
    w_down,
    b_down,
):
    local_images, _, width = patches.shape
    keep_most = keep.shape[1]
    n_dp, n_mp = lax.axis_size("dp"), lax.axis_size("mp")
    d, m = lax.axis_index("dp"), lax.axis_index("mp")
    images_here = local_images * n_mp
    per_slot = (images_here + n_dp - 1) // n_dp
    slot_rows = max(keep_most + 16, per_slot * keep_most * 5 // 8)
    pack_rows = slot_rows * n_dp
    spm = n_dp // n_mp
    feat = width // n_mp
    hc = w_qkv.shape[3]
    place = jnp.stack([m, d]).astype(jnp.int32)

    mixed = join(w_qkv[0], w_o[0].T)
    mixed = lax.all_gather(mixed, "dp", axis=0, tiled=True)
    tokens = embed(place, patches, position, keep, n_mp)
    featured = [tokens[0]] + [hop(tokens[k], k, n_mp) for k in range(1, n_mp)]

    own = mixed[:, :hc]
    quarter = width // 4
    part = jnp.concatenate(
        [lax.dynamic_slice_in_dim(own, (d % 2) * 2 * quarter + i * quarter, quarter) for i in range(2)],
        axis=1,
    )
    mate = [(i, i ^ 1) for i in range(n_dp)]
    out_weights = [[[own]]]
    for pieces in gather_blocks([part], n_mp)[1:]:
        out_weights.append([pieces, [lax.ppermute(p, "dp", mate) for p in pieces]])

    first_image = d * images_here
    group_counts = lax.dynamic_slice_in_dim(counts, first_image, images_here)
    group_offsets = lax.dynamic_slice_in_dim(offsets, first_image, images_here)
    shard_index = group_offsets // pack_rows
    base_row = shard_index * slot_rows + group_offsets - shard_index * pack_rows - d * slot_rows
    spot = jnp.arange(keep_most, dtype=jnp.int32)
    target = jnp.where(
        spot[None, :] < group_counts[:, None], base_row[:, None] + spot[None, :], pack_rows
    ).reshape(n_mp, 1, local_images * keep_most)
    fold = 2
    packed = pack(place, featured, target, n_dp, slot_rows, fold)
    half = n_dp // 2
    bounds = [0, half, n_dp]
    moved = [packed[0]]
    for i in range(1, n_dp):
        moved.append(lax.ppermute(packed[i], "dp", [(j, j ^ i) for j in range(n_dp)]))
    stacks = []
    for i in range(2):
        stacks.append(jnp.stack(moved[bounds[i] : bounds[i + 1]]))
    both = jnp.concatenate([w_up[0], w_down[0].T], axis=1)
    both = lax.all_gather(both, "dp", axis=0, tiled=True)

    image_ids = jnp.arange(counts.shape[0], dtype=jnp.int32)
    slots = jnp.bitwise_xor(jnp.arange(n_dp, dtype=jnp.int32), d)
    packed_rows = d * pack_rows + slots[:, None] * slot_rows + jnp.arange(slot_rows, dtype=jnp.int32)
    packed_rows = packed_rows.reshape(pack_rows)
    inside = (packed_rows[:, None] >= offsets[None, :]) & (
        packed_rows[:, None] < (offsets + counts)[None, :]
    )
    labels = jnp.max(jnp.where(inside, image_ids[None, :] + 1, 0), axis=1) - 1
    labrow = labels.reshape(n_dp, 1, slot_rows)
    labcol = labels.reshape(n_dp, slot_rows, 1)

    moved = [gather_blocks([v], n_mp, i > 0) for i, v in enumerate(stacks)]
    gain = ln_gain[0, 0].reshape(n_mp, 1, feat)
    shift = ln_bias[0, 0].reshape(n_mp, 1, feat)
    bias = b_qkv[0].reshape(1, 3 * hc)
    operands = (mixed, bias, gain, shift, labrow, labcol)
    priors = []
    for i in range(2):
        gathered = [sum(pieces, []) for pieces in zip(*moved[: i + 1])]
        attended = attend(
            place,
            gathered,
            list(range(bounds[i] // spm, bounds[i + 1] // spm)),
            priors if i else [],
            fold,
            hc,
            operands,
            spm,
        )
        priors.append(attended)
    pieces = []
    for s in range(spm):
        pieces.append(
            [attended[0][s]] + [hop(attended[k][s], k, n_mp) for k in range(1, n_mp)]
        )
    base = own_rows(place, gathered, fold, b_o, spm)
    residual, normed = [], []
    last = base[0]
    for s in range(spm):
        kept, last = project(
            place, base[s], hc, pieces[s], out_weights, ln_gain[0, 1:2], ln_bias[0, 1:2], last
        )
        residual.append(kept)
        normed.append(last)
    blocks = gather_blocks(normed, n_mp)
    partials = [[None] * spm for _ in range(n_mp)]
    last = normed[0]
    if n_mp == 4 and spm == 2:
        groups = [[(0, 0), (0, 1)], [(1, 0), (2, 1)], [(1, 1), (2, 0)], [(3, 0), (3, 1)]]
    else:
        groups = [[(k, i) for i in range(spm)] for k in range(n_mp)]
    for group in groups:
        outs = mlp([blocks[k][i] for k, i in group], len(group), both, b_up, last)
        last = outs[0]
        for (k, i), out in zip(group, outs):
            partials[k][i] = out
    early, late = scatter_blocks(partials, n_mp)
    settled = settle(early, residual, b_down)
    own_labels = lax.dynamic_slice_in_dim(labcol, jnp.bitwise_xor(m, d // spm) * spm, spm)
    return finish(place, late, settled, own_labels)


def solution(mesh):
    in_specs = (
        P(("dp", "mp"), None, None),
        P(),
        P(("dp", "mp"), None),
        P(),
        P(),
        P(),
        P(),
        P(None, None, "dp", "mp"),
        P(None, None, "mp"),
        P(None, "mp", "dp"),
        P(),
        P(None, "dp", "mp"),
        P(None, "mp"),
        P(None, "mp", "dp"),
        P(),
    )
    out_specs = P(("dp", "mp"), None)

    return jax.shard_map(
        per_device, mesh=mesh, in_specs=in_specs, out_specs=out_specs, check_vma=False
    )
```
